16 devices in a mesh: frag: 2 (over z), dev: 8 (over y, x, core).
Axes of the slice: x: 2, y: 2, z: 2, core: 2. Of those that a mesh axis runs over, the one named last changes fastest.
Arguments:
- ao_ints: bfloat16 [192, 96, 96, 96], P(('frag', 'dev')), parts along dimension 0
- coeffs: bfloat16 [192, 96], P('frag'), parts along dimension 0
Outputs:
- output: float32 [192, 96, 9216], P('frag', None, 'dev'), parts along dimension 0
There are 2 independent parts. The reference program is written for one: setup_inputs(seed, part) draws one part's arguments, and reference() takes and returns one part's arrays. A program takes and returns all parts, laid end to end along the dimension named above; each array names one.
All inputs are finite; a program needn't handle non-finite values.
Results may differ from the reference program's by a relative error of at most 0.001.
Values are sent between devices in bfloat16 or wider.
A program may use at most 1 GiB of HBM per device.

```python
import jax
import jax.numpy as jnp
from jax import lax

NBASIS = 96


def setup_inputs(seed: int = 0, part: int = 0) -> dict:
    part_key = jax.random.fold_in(jax.random.key(seed), part)
    key_ints, key_coef = jax.random.split(part_key)
    ao_ints = jax.random.normal(key_ints, (NBASIS, NBASIS, NBASIS, NBASIS), jnp.float32).astype(jnp.bfloat16)
    coeffs = (jax.random.normal(key_coef, (NBASIS, NBASIS), jnp.float32) * NBASIS ** -0.5).astype(jnp.bfloat16)
    return {"ao_ints": ao_ints, "coeffs": coeffs}


def reference(ao_ints, coeffs):
    n_basis = coeffs.shape[0]
    coeffs_t = coeffs.T

    def row_transform(a_row):
        a_qsr = jnp.transpose(a_row, (0, 2, 1)).reshape(n_basis * n_basis, n_basis)
        t_one = jnp.dot(a_qsr, coeffs, preferred_element_type=jnp.float32).astype(jnp.bfloat16)
        t_qjs = jnp.transpose(t_one.reshape(n_basis, n_basis, n_basis), (0, 2, 1)).reshape(n_basis * n_basis, n_basis)
        h_row = jnp.dot(t_qjs, coeffs, preferred_element_type=jnp.float32).astype(jnp.bfloat16)
        return jnp.dot(coeffs_t, h_row.reshape(n_basis, n_basis * n_basis), preferred_element_type=jnp.float32).astype(jnp.bfloat16)

    g_all = lax.map(row_transform, ao_ints)
    mo_ints = jnp.dot(coeffs_t, g_all.reshape(n_basis, n_basis ** 3), preferred_element_type=jnp.float32)
    return mo_ints.reshape(n_basis, n_basis, n_basis * n_basis)
```

```python
import jax
import jax.numpy as jnp
from jax import lax
from jax.sharding import PartitionSpec as P

CHUNKS = 4


def solution(mesh):
    n_dev = mesh.shape['dev']

    def local_transform(ao_rows, coeffs):
        local_rows = ao_rows.shape[0]
        n = coeffs.shape[0]
        width = n * n // n_dev
        me = lax.axis_index('dev')
        step = local_rows // CHUNKS
        got = [[None] * CHUNKS for _ in range(n_dev)]
        for c in range(CHUNKS):
            a_c = ao_rows[c * step:(c + 1) * step]
            t_one = jnp.einsum('pqrs,rj->pqsj', a_c, coeffs, preferred_element_type=jnp.float32).astype(jnp.bfloat16)
            half = jnp.einsum('pqsj,sb->pqjb', t_one, coeffs, preferred_element_type=jnp.float32).astype(jnp.bfloat16)
            by_dest = half.reshape(step, n, n_dev, width).transpose(2, 0, 1, 3)
            for k in range(n_dev):
                mine = lax.dynamic_index_in_dim(by_dest, me ^ k, 0, keepdims=False)
                if k:
                    mine = lax.ppermute(mine, 'dev', [(i, i ^ k) for i in range(n_dev)])
                got[k][c] = mine
        full = jnp.concatenate([got[k][c] for k in range(n_dev) for c in range(CHUNKS)], axis=0)
        c_rows = jnp.concatenate(
            [lax.dynamic_slice_in_dim(coeffs, (me ^ k) * local_rows, local_rows, 0) for k in range(n_dev)], axis=0)
        g_local = jnp.einsum('qa,pqk->apk', coeffs, full, preferred_element_type=jnp.float32).astype(jnp.bfloat16)
        return jnp.einsum('pi,apk->iak', c_rows, g_local, preferred_element_type=jnp.float32)

    return jax.shard_map(local_transform, mesh=mesh, in_specs=(P(('frag', 'dev')), P('frag')), out_specs=P('frag', None, 'dev'), check_vma=False)
```

```python
import functools

import jax
import jax.numpy as jnp
from jax import lax
from jax.experimental import pallas as pl
from jax.experimental.pallas import tpu as pltpu
from jax.sharding import PartitionSpec as P

PIECES = ((0, 1, (1152,)), (1, 2, (1152,)), (3, 3, (1152,)), (6, 6, (512, 512, 128)))
TILES = ((0, 512), (512, 512), (1024, 128))
F32, BF16 = jnp.float32, jnp.bfloat16


def one_hot(shape, fn):
    rows = lax.broadcasted_iota(jnp.int32, shape, 0)
    cols = lax.broadcasted_iota(jnp.int32, shape, 1)
    return fn(rows, cols)


def dot(a, b):
    return jnp.dot(a, b, preferred_element_type=F32)


def setup_kernel(n, rows, me_ref, c_ref, ct_ref, l1_ref, r2_ref, l4_ref):
    me = me_ref[0]
    c, ct = c_ref[...], ct_ref[...]
    pick = lambda shape, fn: one_hot(shape, fn).astype(BF16)
    spread = pick((8 * n, n), lambda i, j: i // 8 == j)
    tall = dot(spread, ct).astype(BF16)
    wide = dot(tall, pick((n, 8 * n), lambda i, j: j % n == i))
    keep = one_hot((8 * n, 8 * n), lambda i, j: i % 8 == j // n)
    l1_ref[...] = jnp.where(keep, wide, 0.0).astype(BF16)

    def source(r, col):
        m = col // 8
        return r == (me ^ (m // rows)) * rows + m % rows
    wide = dot(tall, pick((n, 8 * n), source))
    keep = one_hot((8 * n, 8 * n), lambda i, j: i % 8 == j % 8)
    l4_ref[...] = jnp.where(keep, wide, 0.0).astype(BF16)
    tall = dot(pick((512, n), lambda i, j: i % 128 == j), c).astype(BF16)
    wide = dot(tall, pick((n, 4 * n), lambda i, j: j % n == i))
    keep = one_hot((512, 4 * n), lambda i, j: i // 128 == j // n)
    r2_ref[...] = jnp.where(keep, wide, 0.0).astype(BF16)


def send_kernel(n, n_dev, tiles, me_ref, a_ref, l1_ref, r2_ref, ct_ref, *rest):
    outs, t1_ref = rest[-1 - n_dev * len(tiles):-1], rest[-1]
    nj = n // n_dev
    me = me_ref[0]

    @pl.when(pl.program_id(0) == 0)
    def _():
        t1_ref[...] = jnp.zeros_like(t1_ref)

    def first(g, carry):
        q0 = pl.multiple_of(g * 16, 16)
        lo = dot(l1_ref[...], a_ref[0, pl.ds(q0, 8)].reshape(8 * n, n))
        hi = dot(l1_ref[...], a_ref[0, pl.ds(q0 + 8, 8)].reshape(8 * n, n))
        both = jnp.concatenate([lo.reshape(n, 8, n), hi.reshape(n, 8, n)], axis=1)
        t1_ref[:, pl.ds(q0, 16), :n] = both.astype(BF16)
        return carry

    lax.fori_loop(0, n // 16, first, 0)
    for k in range(n_dev):
        d = me ^ k
        t = t1_ref[pl.ds(d * nj, nj)].reshape(nj // 4, 4, n, 128)
        lhs = jnp.concatenate([t[:, jj].reshape(nj // 4 * n, 128) for jj in range(4)], axis=1)
        h = dot(lhs, r2_ref[...]).astype(BF16)
        h = jnp.concatenate([h[g * n:(g + 1) * n] for g in range(nj // 4)], axis=1)
        g = dot(ct_ref[...], h).astype(BF16)
        off = 0
        for t_i, w in enumerate(tiles):
            outs[k * len(tiles) + t_i][0] = g[:, off:off + w]
            off += w


def out_kernel(n, n_in, width, *refs):
    l4_ref, out_ref = refs[n_in], refs[-1]
    rhs = jnp.concatenate([r[...].reshape(-1, width) for r in refs[:n_in]], axis=0)
    out_ref[...] = dot(l4_ref[...], rhs).reshape(n, 8, width)


def solution(mesh):
    n_dev = mesh.shape['dev']

    def local_transform(ao_rows, coeffs):
        rows = ao_rows.shape[0]
        n = coeffs.shape[0]
        wide = n * n // n_dev
        me = lax.axis_index('dev')
        me_arr = jnp.full((1,), me, jnp.int32)
        ct = coeffs.T
        smem = pl.BlockSpec(memory_space=pltpu.SMEM)
        vmem = pl.BlockSpec(memory_space=pltpu.VMEM)
        l1, r2, l4 = pl.pallas_call(
            functools.partial(setup_kernel, n, rows),
            in_specs=[smem, vmem, vmem],
            out_specs=[vmem] * 3,
            out_shape=[jax.ShapeDtypeStruct(s, BF16) for s in ((8 * n, 8 * n), (512, 4 * n), (8 * n, 8 * n))],
            name='setup',
        )(me_arr, coeffs, ct)

        def const(shape):
            return pl.BlockSpec(shape, lambda *_: (0,) * len(shape))

        got = [[] for _ in range(n_dev)]
        before = []
        for p0, count, tiles in PIECES:
            sent = pl.pallas_call(
                functools.partial(send_kernel, n, n_dev, tiles),
                grid=(count,),
                in_specs=[smem, pl.BlockSpec((1, n, n, n), lambda i, p0=p0: (p0 + i, 0, 0, 0)),
                          const((8 * n, 8 * n)), const((512, 4 * n)), const((n, n))]
                + [pl.BlockSpec(memory_space=pl.ANY)] * len(before),
                out_specs=[pl.BlockSpec((1, n, w), lambda i: (i, 0, 0)) for _ in range(n_dev) for w in tiles],
                out_shape=[jax.ShapeDtypeStruct((count, n, w), BF16) for _ in range(n_dev) for w in tiles],
                scratch_shapes=[pltpu.VMEM((n, n, 128), BF16)],
                cost_estimate=pl.CostEstimate(flops=count * 6 * n ** 4, bytes_accessed=count * 4 * n ** 3, transcendentals=0),
                name='send',
            )(me_arr, ao_rows, l1, r2, ct, *before)
            before = [sent[0]]
            for t_i in range(len(tiles)):
                for k in range(n_dev):
                    block = sent[k * len(tiles) + t_i]
                    if k:
                        block = lax.ppermute(block, 'dev', [(i, i ^ k) for i in range(n_dev)])
                    got[k].append((block, t_i if len(tiles) > 1 else None))

        out = None
        for t_i, (off, w) in enumerate(TILES):
            ins, specs = [], []
            for k in range(n_dev):
                for block, tile in got[k]:
                    if tile in (None, t_i):
                        lane = off // w if tile is None else 0
                        ins.append(block)
                        specs.append(pl.BlockSpec((block.shape[0], 8, w), lambda i, lane=lane: (0, i, lane)))
            n_in = len(ins)
            ins.append(l4)
            specs.append(const((8 * n, 8 * n)))
            if out is not None:
                ins.append(out)
                specs.append(pl.BlockSpec(memory_space=pl.ANY))
            out = pl.pallas_call(
                functools.partial(out_kernel, n, n_in, w),
                grid=(n // 8,),
                in_specs=specs,
                out_specs=pl.BlockSpec((n, 8, w), lambda i, off=off, w=w: (0, i, off // w)),
                out_shape=jax.ShapeDtypeStruct((n, n, wide), F32),
                input_output_aliases={} if t_i == 0 else {len(ins) - 1: 0},
                cost_estimate=pl.CostEstimate(flops=2 * n ** 3 * w, bytes_accessed=6 * n * n * w, transcendentals=0),
                name='out',
            )(*ins)
        return out

    return jax.shard_map(local_transform, mesh=mesh, in_specs=(P(('frag', 'dev')), P('frag')), out_specs=P('frag', None, 'dev'), check_vma=False)
```

```python
import functools

import jax
import jax.numpy as jnp
from jax import lax
from jax.experimental import pallas as pl
from jax.experimental.pallas import tpu as pltpu
from jax.sharding import PartitionSpec as P


PIECES = ((0, 1, (1152,)), (1, 1, (1152,)), (2, 2, (1152,)), (4, 3, (1152,)), (7, 5, (512, 512, 128)))
TILES = ((0, 512, 32, 1), (512, 512, 32, 1), (1024, 128, 32, 2))
F32, BF16 = jnp.float32, jnp.bfloat16


def one_hot(shape, fn):
    rows = lax.broadcasted_iota(jnp.int32, shape, 0)
    cols = lax.broadcasted_iota(jnp.int32, shape, 1)
    return fn(rows, cols)


def dot(a, b):
    return jnp.dot(a, b, preferred_element_type=F32)


def pick(shape, fn):
    return one_hot(shape, fn).astype(BF16)


def transposed(c, n):
    eye = pick((n, n), lambda i, j: i == j)
    return lax.dot_general(c, eye, (((0,), (0,)), ((), ())), preferred_element_type=F32).astype(BF16)


def build_first(n, c_ref, l1_ref, r2_ref, ct_ref):
    c = c_ref[...]
    ct = transposed(c, n)
    ct_ref[...] = ct
    tall = dot(pick((8 * n, n), lambda i, j: i // 8 == j), ct).astype(BF16)
    wide = dot(tall, pick((n, 8 * n), lambda i, j: j % n == i))
    keep = one_hot((8 * n, 8 * n), lambda i, j: i % 8 == j // n)
    l1_ref[...] = jnp.where(keep, wide, 0.0).astype(BF16)
    tall = dot(pick((512, n), lambda i, j: i % 128 == j), c).astype(BF16)
    wide = dot(tall, pick((n, 4 * n), lambda i, j: j % n == i))
    keep = one_hot((512, 4 * n), lambda i, j: i // 128 == j // n)
    r2_ref[...] = jnp.where(keep, wide, 0.0).astype(BF16)


def build_last(n, rows, me, ct_ref, l4_ref):
    def source(r, col):
        m = col // 8
        return r == (me ^ (m // rows)) * rows + m % rows

    tall = dot(pick((8 * n, n), lambda i, j: i // 8 == j), ct_ref[...]).astype(BF16)
    wide = dot(tall, pick((n, 8 * n), source))
    keep = one_hot((8 * n, 8 * n), lambda i, j: i % 8 == j % 8)
    l4_ref[...] = jnp.where(keep, wide, 0.0).astype(BF16)


def one_row(n, n_dev, tiles, me, a_ref, l1_ref, r2_ref, ct_ref, outs, t1_ref):
    nj = n // n_dev
    zero = jnp.zeros((8 * n, 128 - n), BF16)

    def first(g, carry):
        q0 = pl.multiple_of(g * 16, 16)
        lo = a_ref[pl.ds(q0, 8)].reshape(8 * n, n)
        hi = a_ref[pl.ds(q0 + 8, 8)].reshape(8 * n, n)
        t = dot(l1_ref[...], jnp.concatenate([lo, zero, hi, zero], axis=1))
        both = jnp.concatenate([t[:, :128].reshape(n, 8, 128), t[:, 128:].reshape(n, 8, 128)], axis=1)
        t1_ref[:, pl.ds(q0, 16), :] = both.astype(BF16)
        return carry

    lax.fori_loop(0, n // 16, first, 0)
    for k in range(n_dev):
        d = me ^ k
        t = t1_ref[pl.ds(d * nj, nj)].reshape(nj // 4, 4, n, 128)
        lhs = jnp.concatenate([t[:, jj].reshape(nj // 4 * n, 128) for jj in range(4)], axis=1)
        h = dot(lhs, r2_ref[...]).astype(BF16)
        h = jnp.concatenate([h[g * n:(g + 1) * n] for g in range(nj // 4)], axis=1)
        g = dot(ct_ref[...], h).astype(BF16)
        off = 0
        for t_i, w in enumerate(tiles):
            outs[k * len(tiles) + t_i][0] = g[:, off:off + w]
            off += w


def first_kernel(n, n_dev, tiles, me_ref, a_hbm, c_ref, l1_ref, r2_ref, ct_ref, *rest):
    outs, (a_buf, t1_ref, sem) = rest[:-3], rest[-3:]
    copy = pltpu.make_async_copy(a_hbm.at[0], a_buf, sem)
    copy.start()
    build_first(n, c_ref, l1_ref, r2_ref, ct_ref)
    copy.wait()
    one_row(n, n_dev, tiles, me_ref[0], a_buf, l1_ref, r2_ref, ct_ref, outs, t1_ref)


def send_kernel(n, n_dev, rows, tiles, last, me_ref, a_ref, l1_ref, r2_ref, ct_ref, before, *rest):
    outs, t1_ref = rest[:n_dev * len(tiles)], rest[-1]
    one_row(n, n_dev, tiles, me_ref[0], a_ref.at[0], l1_ref, r2_ref, ct_ref, outs, t1_ref)
    if last:
        @pl.when(pl.program_id(0) == 0)
        def _():
            build_last(n, rows, me_ref[0], ct_ref, rest[-2])


def out_kernel(n, n_in, width, depth, pack, *refs):
    l4_ref, out_ref = refs[n_in], refs[-1]
    ins = refs[:n_in]

    def step(s, carry):
        a0 = pl.multiple_of(s * 8 * pack, 8 * pack)
        cols = []
        for x in range(pack):
            cols.append(jnp.concatenate(
                [r[:, pl.ds(a0 + 8 * x, 8), :].reshape(-1, width) for r in ins], axis=0))
        rhs = cols[0] if pack == 1 else jnp.concatenate(cols, axis=1)
        v = dot(l4_ref[...], rhs)
        for x in range(pack):
            out_ref[:, pl.ds(a0 + 8 * x, 8), :] = v[:, x * width:(x + 1) * width].reshape(n, 8, width)
        return carry

    lax.fori_loop(0, depth // (8 * pack), step, 0)


def solution(mesh):
    n_dev = mesh.shape['dev']

    def transform(ao_rows, coeffs):
        rows = ao_rows.shape[0]
        n = coeffs.shape[0]
        wide = n * n // n_dev
        me_arr = jnp.full((1,), lax.axis_index('dev'), jnp.int32)
        smem = pl.BlockSpec(memory_space=pltpu.SMEM)
        vmem = pl.BlockSpec(memory_space=pltpu.VMEM)
        hbm = pl.BlockSpec(memory_space=pl.ANY)

        def const(shape):
            return pl.BlockSpec(shape, lambda *_: (0,) * len(shape))

        square, second = (8 * n, 8 * n), (512, 4 * n)
        got = [[] for _ in range(n_dev)]
        for i, (p0, count, tiles) in enumerate(PIECES):
            block_specs = [pl.BlockSpec((1, n, w), lambda i: (i, 0, 0)) for _ in range(n_dev) for w in tiles]
            block_shapes = [jax.ShapeDtypeStruct((count, n, w), BF16) for _ in range(n_dev) for w in tiles]
            t1 = pltpu.VMEM((n, n, 128), BF16)
            if i == 0:
                l1, r2, ct, *sent = pl.pallas_call(
                    functools.partial(first_kernel, n, n_dev, tiles),
                    grid=(1,),
                    in_specs=[smem, hbm, vmem],
                    out_specs=[const(square), const(second), const((n, n))] + block_specs,
                    out_shape=[jax.ShapeDtypeStruct(s, BF16) for s in (square, second, (n, n))] + block_shapes,
                    scratch_shapes=[pltpu.VMEM((n, n, n), BF16), t1, pltpu.SemaphoreType.DMA],
                    name='first',
                )(me_arr, ao_rows, coeffs)
            else:
                last = i == 1
                sent = pl.pallas_call(
                    functools.partial(send_kernel, n, n_dev, rows, tiles, last),
                    grid=(count,),
                    in_specs=[smem, pl.BlockSpec((1, n, n, n), lambda i, p0=p0: (p0 + i, 0, 0, 0)),
                              const(square), const(second), const((n, n)), hbm],
                    out_specs=block_specs + [const(square)] * last,
                    out_shape=block_shapes + [jax.ShapeDtypeStruct(square, BF16)] * last,
                    scratch_shapes=[t1],
                    name='send',
                )(me_arr, ao_rows, l1, r2, ct, before)
                if last:
                    l4 = sent[-1]
            before = sent[0]
            for t_i in range(len(tiles)):
                for k in range(n_dev):
                    block = sent[k * len(tiles) + t_i]
                    if k:
                        block = lax.ppermute(block, 'dev', [(i, i ^ k) for i in range(n_dev)])
                    got[k].append((block, t_i if len(tiles) > 1 else None))

        out = None
        for t_i, (off, w, depth, pack) in enumerate(TILES):
            ins, specs = [], []
            for k in range(n_dev):
                for block, tile in got[k]:
                    if tile in (None, t_i):
                        lane = off // w if tile is None else 0
                        ins.append(block)
                        specs.append(pl.BlockSpec((block.shape[0], depth, w), lambda i, lane=lane: (0, i, lane)))
            n_in = len(ins)
            ins.append(l4)
            specs.append(const(square))
            if out is not None:
                ins.append(out)
                specs.append(hbm)
            out = pl.pallas_call(
                functools.partial(out_kernel, n, n_in, w, depth, pack),
                grid=(n // depth,),
                in_specs=specs,
                out_specs=pl.BlockSpec((n, depth, w), lambda i, off=off, w=w: (0, i, off // w)),
                out_shape=jax.ShapeDtypeStruct((n, n, wide), F32),
                input_output_aliases={} if t_i == 0 else {len(ins) - 1: 0},
                name='out',
            )(*ins)
        return out

    return jax.shard_map(transform, mesh=mesh, in_specs=(P(('frag', 'dev')), P('frag')), out_specs=P('frag', None, 'dev'), check_vma=False)
```

```python
import functools

import jax
import jax.numpy as jnp
from jax import lax
from jax.experimental import pallas as pl
from jax.experimental.pallas import tpu as pltpu
from jax.sharding import PartitionSpec as P


PIECES = ((0, 2, (96,)), (2, 4, (96,)), (6, 6, (40, 32, 16, 8)))
TILES = ((0, 40), (40, 32), (72, 16), (88, 8))
F32, BF16 = jnp.float32, jnp.bfloat16


def one_hot(shape, fn):
    rows = lax.broadcasted_iota(jnp.int32, shape, 0)
    cols = lax.broadcasted_iota(jnp.int32, shape, 1)
    return fn(rows, cols)


def dot(a, b):
    return jnp.dot(a, b, preferred_element_type=F32)


def pick(shape, fn):
    return one_hot(shape, fn).astype(BF16)


def transposed(c, n):
    eye = pick((n, n), lambda i, j: i == j)
    return lax.dot_general(c, eye, (((0,), (0,)), ((), ())), preferred_element_type=F32).astype(BF16)


def build_first(n, c_ref, l1_ref, r2_ref, ct_ref):
    c = c_ref[...]
    ct = transposed(c, n)
    ct_ref[...] = ct
    tall = dot(pick((8 * n, n), lambda i, j: i // 8 == j), ct).astype(BF16)
    wide = dot(tall, pick((n, 8 * n), lambda i, j: j % n == i))
    keep = one_hot((8 * n, 8 * n), lambda i, j: i % 8 == j // n)
    l1_ref[...] = jnp.where(keep, wide, 0.0).astype(BF16)
    tall = dot(pick((512, n), lambda i, j: i % 128 == j), c).astype(BF16)
    wide = dot(tall, pick((n, 4 * n), lambda i, j: j % n == i))
    keep = one_hot((512, 4 * n), lambda i, j: i // 128 == j // n)
    r2_ref[...] = jnp.where(keep, wide, 0.0).astype(BF16)


def build_last(n, rows, me, ct_ref, l4_ref):
    def source(r, col):
        m = col // 8
        return r == (me ^ (m // rows)) * rows + m % rows

    tall = dot(pick((8 * n, n), lambda i, j: i // 8 == j), ct_ref[...]).astype(BF16)
    wide = dot(tall, pick((n, 8 * n), source))
    keep = one_hot((8 * n, 8 * n), lambda i, j: i % 8 == j % 8)
    l4_ref[...] = jnp.where(keep, wide, 0.0).astype(BF16)


def one_row(n, n_dev, tiles, me, a_ref, l1_ref, r2_ref, ct_ref, outs, t1_ref, row):
    nj = n // n_dev
    zero = jnp.zeros((8 * n, 128 - n), BF16)

    def first(g, carry):
        q0 = pl.multiple_of(g * 16, 16)
        lo = a_ref[pl.ds(q0, 8)].reshape(8 * n, n)
        hi = a_ref[pl.ds(q0 + 8, 8)].reshape(8 * n, n)
        t = dot(l1_ref[...], jnp.concatenate([lo, zero, hi, zero], axis=1))
        both = jnp.concatenate([t[:, :128].reshape(n, 8, 128), t[:, 128:].reshape(n, 8, 128)], axis=1)
        t1_ref[:, pl.ds(q0, 16), :] = both.astype(BF16)
        return carry

    lax.fori_loop(0, n // 16, first, 0)
    for k in range(n_dev):
        d = me ^ k
        t = t1_ref[pl.ds(d * nj, nj)].reshape(nj // 4, 4, n, 128)
        lhs = jnp.concatenate([t[:, jj].reshape(nj // 4 * n, 128) for jj in range(4)], axis=1)
        h = dot(lhs, r2_ref[...]).astype(BF16)
        h = jnp.concatenate([h[g * n:(g + 1) * n] for g in range(nj // 4)], axis=1)
        g = dot(ct_ref[...], h).astype(BF16)
        off = 0
        for t_i, w in enumerate(tiles):
            outs[k * len(tiles) + t_i][row] = g[off:off + w]
            off += w


def first_kernel(n, n_dev, count, tiles, me_ref, a_hbm, c_ref, l1_ref, r2_ref, ct_ref, *rest):
    outs, (a_buf, t1_ref, sem) = rest[:-3], rest[-3:]
    copies = [pltpu.make_async_copy(a_hbm.at[i], a_buf.at[i], sem.at[i]) for i in range(count)]
    for copy in copies:
        copy.start()
    build_first(n, c_ref, l1_ref, r2_ref, ct_ref)

    def row(i, carry):
        pltpu.make_async_copy(a_hbm.at[i], a_buf.at[i], sem.at[i]).wait()
        one_row(n, n_dev, tiles, me_ref[0], a_buf.at[i], l1_ref, r2_ref, ct_ref, outs, t1_ref, i)
        return carry

    lax.fori_loop(0, count, row, 0)


def send_kernel(n, n_dev, rows, tiles, last, me_ref, a_ref, l1_ref, r2_ref, ct_ref, before, *rest):
    outs, t1_ref = rest[:n_dev * len(tiles)], rest[-1]
    one_row(n, n_dev, tiles, me_ref[0], a_ref.at[0], l1_ref, r2_ref, ct_ref, outs, t1_ref, 0)
    if last:
        @pl.when(pl.program_id(0) == 0)
        def _():
            build_last(n, rows, me_ref[0], ct_ref, rest[-2])


def out_kernel(n, n_in, wide, *refs):
    l4_ref, out_ref = refs[n_in], refs[-1]
    rhs = jnp.concatenate([r[...].reshape(-1, wide) for r in refs[:n_in]], axis=0)
    out_ref[...] = dot(l4_ref[...], rhs).reshape(n, 8, wide)


def solution(mesh):
    n_dev = mesh.shape['dev']

    def transform(ao_rows, coeffs):
        rows = ao_rows.shape[0]
        n = coeffs.shape[0]
        wide = n * n // n_dev
        me_arr = jnp.full((1,), lax.axis_index('dev'), jnp.int32)
        smem = pl.BlockSpec(memory_space=pltpu.SMEM)
        vmem = pl.BlockSpec(memory_space=pltpu.VMEM)
        hbm = pl.BlockSpec(memory_space=pl.ANY)

        def const(shape):
            return pl.BlockSpec(shape, lambda *_: (0,) * len(shape))

        square, second = (8 * n, 8 * n), (512, 4 * n)
        got = [[] for _ in range(n_dev)]
        for i, (p0, count, tiles) in enumerate(PIECES):
            block_specs = [pl.BlockSpec((count if i == 0 else 1, w, wide), lambda i: (i, 0, 0)) for _ in range(n_dev) for w in tiles]
            block_shapes = [jax.ShapeDtypeStruct((count, w, wide), BF16) for _ in range(n_dev) for w in tiles]
            t1 = pltpu.VMEM((n, n, 128), BF16)
            if i == 0:
                l1, r2, ct, *sent = pl.pallas_call(
                    functools.partial(first_kernel, n, n_dev, count, tiles),
                    grid=(1,),
                    in_specs=[smem, hbm, vmem],
                    out_specs=[const(square), const(second), const((n, n))] + block_specs,
                    out_shape=[jax.ShapeDtypeStruct(s, BF16) for s in (square, second, (n, n))] + block_shapes,
                    scratch_shapes=[pltpu.VMEM((count, n, n, n), BF16), t1, pltpu.SemaphoreType.DMA((count,))],
                    name='first',
                )(me_arr, ao_rows, coeffs)
            else:
                last = i == 1
                sent = pl.pallas_call(
                    functools.partial(send_kernel, n, n_dev, rows, tiles, last),
                    grid=(count,),
                    in_specs=[smem, pl.BlockSpec((1, n, n, n), lambda i, p0=p0: (p0 + i, 0, 0, 0)),
                              const(square), const(second), const((n, n)), hbm],
                    out_specs=block_specs + [const(square)] * last,
                    out_shape=block_shapes + [jax.ShapeDtypeStruct(square, BF16)] * last,
                    scratch_shapes=[t1],
                    name='send',
                )(me_arr, ao_rows, l1, r2, ct, before)
                if last:
                    l4 = sent[-1]
            before = sent[0]
            for t_i in range(len(tiles)):
                for k in range(n_dev):
                    block = sent[k * len(tiles) + t_i]
                    if k:
                        block = lax.ppermute(block, 'dev', [(i, i ^ k) for i in range(n_dev)])
                    got[k].append((block, t_i if len(tiles) > 1 else None))

        out = None
        for t_i, (a0, size) in enumerate(TILES):
            ins, specs = [], []
            for k in range(n_dev):
                for block, tile in got[k]:
                    if tile in (None, t_i):
                        base = a0 // 8 if tile is None else 0
                        ins.append(block)
                        specs.append(pl.BlockSpec((block.shape[0], 8, wide), lambda i, base=base: (0, base + i, 0)))
            n_in = len(ins)
            ins.append(l4)
            specs.append(const(square))
            if out is not None:
                ins.append(out)
                specs.append(hbm)
            out = pl.pallas_call(
                functools.partial(out_kernel, n, n_in, wide),
                grid=(size // 8,),
                in_specs=specs,
                out_specs=pl.BlockSpec((n, 8, wide), lambda i, a0=a0: (0, a0 // 8 + i, 0)),
                out_shape=jax.ShapeDtypeStruct((n, n, wide), F32),
                input_output_aliases={} if t_i == 0 else {len(ins) - 1: 0},
                name='out',
            )(*ins)
        return out

    return jax.shard_map(transform, mesh=mesh, in_specs=(P(('frag', 'dev')), P('frag')), out_specs=P('frag', None, 'dev'), check_vma=False)
```

```python
import functools

import jax
import jax.numpy as jnp
from jax import lax
from jax.experimental import pallas as pl
from jax.experimental.pallas import tpu as pltpu
from jax.sharding import PartitionSpec as P


TILES = ((0, 48, 0, 1152), (48, 24, 0, 1152), (72, 8, 0, 1152), (80, 8, 0, 1152), (88, 8, 0, 768), (88, 8, 768, 384))
DIAGONAL = (6, 7)
DIRECT = (2, 4, 3, 5, 1)
F32, BF16 = jnp.float32, jnp.bfloat16


def one_hot(shape, fn):
    rows = lax.broadcasted_iota(jnp.int32, shape, 0)
    cols = lax.broadcasted_iota(jnp.int32, shape, 1)
    return fn(rows, cols)


def dot(a, b):
    return jnp.dot(a, b, preferred_element_type=F32)


def pick(shape, fn):
    return one_hot(shape, fn).astype(BF16)


def transposed(c, n):
    eye = pick((n, n), lambda i, j: i == j)
    return lax.dot_general(c, eye, (((0,), (0,)), ((), ())), preferred_element_type=F32).astype(BF16)


def build_first(n, c_ref, l1_ref, r2_ref, ct_ref):
    c = c_ref[...]
    ct = transposed(c, n)
    ct_ref[...] = ct
    tall = dot(pick((8 * n, n), lambda i, j: i // 8 == j), ct).astype(BF16)
    wide = dot(tall, pick((n, 8 * n), lambda i, j: j % n == i))
    keep = one_hot((8 * n, 8 * n), lambda i, j: i % 8 == j // n)
    l1_ref[...] = jnp.where(keep, wide, 0.0).astype(BF16)
    tall = dot(pick((512, n), lambda i, j: i % 128 == j), c).astype(BF16)
    wide = dot(tall, pick((n, 4 * n), lambda i, j: j % n == i))
    keep = one_hot((512, 4 * n), lambda i, j: i // 128 == j // n)
    r2_ref[...] = jnp.where(keep, wide, 0.0).astype(BF16)


def last_kernel(n, rows, me_ref, c_ref, after_ref, l4_ref):
    me = me_ref[0]

    def source(r, col):
        m = col // 8
        return r == (me ^ (m // rows)) * rows + m % rows

    ct = transposed(c_ref[...], n)
    tall = dot(pick((8 * n, n), lambda i, j: i // 8 == j), ct).astype(BF16)
    wide = dot(tall, pick((n, 8 * n), source))
    keep = one_hot((8 * n, 8 * n), lambda i, j: i % 8 == j % 8)
    l4_ref[...] = jnp.where(keep, wide, 0.0).astype(BF16)


def flipped(me, k):
    out = 0
    for bit in (1, 2, 4):
        b = (me // bit) % 2
        out = out + bit * (1 - b if k & bit else b)
    return out


def exchange_kernel(n, n_dev, rows, a_hbm, c_ref, *refs):
    n_got, n_tile = n_dev - len(DIAGONAL), len(TILES)
    got, tiles = refs[:n_got], refs[n_got:n_got + len(DIAGONAL) * n_tile]
    (a_buf, t1_ref, g_ref, l1_ref, r2_ref, ct_ref, a_sem, chunk_sem, own_sem, tile_sem, send_sem,
     recv_sem) = refs[n_got + len(tiles):]
    nj = n // n_dev
    me = lax.axis_index('dev')
    barrier = pltpu.get_barrier_semaphore()
    for k in DIRECT:
        pl.semaphore_signal(barrier, inc=1, device_id={'dev': flipped(me, k)}, device_id_type=pl.DeviceIdType.MESH)

    def chunk(g):
        q = pl.ds(g * 16, 16)
        return pltpu.make_async_copy(a_hbm.at[0, q], a_buf.at[0, q], chunk_sem.at[g])

    def fetch(i):
        slot = lax.rem(i, 2)
        return pltpu.make_async_copy(a_hbm.at[i], a_buf.at[slot], a_sem.at[slot])

    for g in range(n // 16):
        chunk(g).start()
    fetch(1).start()
    build_first(n, c_ref, l1_ref, r2_ref, ct_ref)
    zero = jnp.zeros((8 * n, 128 - n), BF16)

    def remote(k, src, dst):
        return pltpu.make_async_remote_copy(
            src_ref=src, dst_ref=dst, send_sem=send_sem.at[k], recv_sem=recv_sem.at[k],
            device_id={'dev': flipped(me, k)}, device_id_type=pl.DeviceIdType.MESH)

    def tile_copies(k, rows_):
        x = DIAGONAL.index(k)
        for t, (a0, size, lane, lanes) in enumerate(TILES):
            j = x * n_tile + t
            src = g_ref.at[k, rows_, pl.ds(a0, size), pl.ds(lane, lanes)]
            yield pltpu.make_async_copy(src, tiles[j].at[rows_], tile_sem.at[j])

    def send(k, i):
        if k == 0:
            pltpu.make_async_copy(g_ref.at[0, i], got[0].at[i], own_sem).start()
        elif k in DIAGONAL:
            for copy in tile_copies(k, i):
                copy.start()
        else:
            remote(k, g_ref.at[k, i], got[k].at[i]).start()

    def step_one(slot, g, lhs):
        q0 = pl.multiple_of(g * 16, 16)
        lo = a_buf[slot, pl.ds(q0, 8)].reshape(8 * n, n)
        hi = a_buf[slot, pl.ds(q0 + 8, 8)].reshape(8 * n, n)
        t = dot(lhs, jnp.concatenate([lo, zero, hi, zero], axis=1))
        nj = t.shape[0] // 8
        t = jnp.concatenate([t[:, :128].reshape(nj, 8, 128), t[:, 128:].reshape(nj, 8, 128)], axis=1)
        return pl.ds(q0, 16), t.astype(BF16)

    def step_two_three(k, i):
        d = flipped(me, k)
        t = t1_ref[pl.ds(d * nj, nj)].reshape(nj // 4, 4, n, 128)
        lhs = jnp.concatenate([t[:, jj].reshape(nj // 4 * n, 128) for jj in range(4)], axis=1)
        h = dot(lhs, r2_ref[...]).astype(BF16)
        h = jnp.concatenate([h[g * n:(g + 1) * n] for g in range(nj // 4)], axis=1)
        g_ref[k, i] = dot(ct_ref[...], h).astype(BF16)

    def some(ks, i, slot, wait):
        def first(g, carry):
            if wait:
                chunk(g).wait()
            lhs = jnp.concatenate(
                [l1_ref[pl.ds(pl.multiple_of(flipped(me, k) * 8 * nj, 8 * nj), 8 * nj)] for k in ks], axis=0)
            q, t = step_one(slot, g, lhs)
            for x, k in enumerate(ks):
                t1_ref[pl.ds(flipped(me, k) * nj, nj), q, :] = t[x * nj:(x + 1) * nj]
            return carry

        lax.fori_loop(0, n // 16, first, 0)
        for k in ks:
            step_two_three(k, i)

    some(DIRECT[:2], 0, 0, True)
    pl.semaphore_wait(barrier, len(DIRECT))
    for k in DIRECT[:2]:
        send(k, 0)
    some((*DIRECT[2:], 0, *DIAGONAL), 0, 0, False)
    for k in (*DIRECT[2:], 0, *DIAGONAL):
        send(k, 0)

    def row(i, carry):
        slot = lax.rem(i, 2)
        fetch(i).wait()

        @pl.when(i + 1 < rows)
        def _():
            fetch(i + 1).start()

        def first(g, carry):
            q, t = step_one(slot, g, l1_ref[...])
            t1_ref[:, q, :] = t
            return carry

        lax.fori_loop(0, n // 16, first, 0)
        before = None
        for k in (*DIRECT, 0, *DIAGONAL):
            step_two_three(k, i)
            if before is not None:
                send(before, i)
            before = k
        send(before, i)
        return carry

    lax.fori_loop(1, rows, row, 0)
    pltpu.make_async_copy(g_ref.at[0], got[0], own_sem).wait()
    for k in DIAGONAL:
        for copy in tile_copies(k, pl.ds(0, rows)):
            copy.wait()
    for k in DIRECT:
        remote(k, g_ref.at[k], got[k]).wait()


def out_kernel(n, n_in, wide, *refs):
    l4_ref, out_ref = refs[n_in], refs[-1]
    rhs = jnp.concatenate([r[...].reshape(-1, wide) for r in refs[:n_in]], axis=0)
    out_ref[...] = dot(l4_ref[...], rhs).reshape(n, 8, wide)


def solution(mesh):
    n_dev = mesh.shape['dev']

    def transform(ao_rows, coeffs):
        rows = ao_rows.shape[0]
        n = coeffs.shape[0]
        wide = n * n // n_dev
        me_arr = jnp.full((1,), lax.axis_index('dev'), jnp.int32)
        smem = pl.BlockSpec(memory_space=pltpu.SMEM)
        vmem = pl.BlockSpec(memory_space=pltpu.VMEM)
        hbm = pl.BlockSpec(memory_space=pl.ANY)

        def const(shape):
            return pl.BlockSpec(shape, lambda *_: (0,) * len(shape))

        square, second = (8 * n, 8 * n), (512, 4 * n)
        n_got = n_dev - len(DIAGONAL)
        shapes = [(rows, n, wide)] * n_got
        shapes += [(rows, size, lanes) for _ in DIAGONAL for _, size, _, lanes in TILES]
        outs = pl.pallas_call(
            functools.partial(exchange_kernel, n, n_dev, rows),
            in_specs=[hbm, vmem],
            out_specs=[hbm] * len(shapes),
            out_shape=[jax.ShapeDtypeStruct(s, BF16) for s in shapes],
            scratch_shapes=[
                pltpu.VMEM((2, n, n, n), BF16), pltpu.VMEM((n, n, 128), BF16),
                pltpu.VMEM((n_dev, rows, n, wide), BF16), pltpu.VMEM(square, BF16),
                pltpu.VMEM(second, BF16), pltpu.VMEM((n, n), BF16),
                pltpu.SemaphoreType.DMA((2,)), pltpu.SemaphoreType.DMA((n // 16,)), pltpu.SemaphoreType.DMA,
                pltpu.SemaphoreType.DMA((len(shapes) - n_got,)),
                pltpu.SemaphoreType.DMA((n_dev,)), pltpu.SemaphoreType.DMA((n_dev,))],
            compiler_params=pltpu.CompilerParams(collective_id=0, has_side_effects=True),
            name='exchange',
        )(ao_rows, coeffs)
        got, tiles = outs[:n_got], outs[n_got:]
        moved = {}
        for t in range(len(TILES)):
            for x, k in enumerate(DIAGONAL):
                moved[k, t] = lax.ppermute(
                    tiles[x * len(TILES) + t], 'dev', [(i, i ^ k) for i in range(n_dev)])
        l4 = pl.pallas_call(
            functools.partial(last_kernel, n, rows),
            in_specs=[smem, vmem, hbm],
            out_specs=vmem,
            out_shape=jax.ShapeDtypeStruct(square, BF16),
            name='last',
        )(me_arr, coeffs, got[0])

        out = None
        for t_i, (a0, size, lane, lanes) in enumerate(TILES):
            ins, specs = [], []
            for k in range(n_dev):
                block, at = (moved[k, t_i], (0, 0)) if (k, t_i) in moved else (got[k], (a0 // 8, lane // lanes))
                ins.append(block)
                specs.append(pl.BlockSpec((rows, 8, lanes), lambda i, at=at: (0, at[0] + i, at[1])))
            n_in = len(ins)
            ins.append(l4)
            specs.append(const(square))
            if out is not None:
                ins.append(out)
                specs.append(hbm)
            out = pl.pallas_call(
                functools.partial(out_kernel, n, n_in, lanes),
                grid=(size // 8,),
                in_specs=specs,
                out_specs=pl.BlockSpec((n, 8, lanes), lambda i, at=(a0 // 8, lane // lanes): (0, at[0] + i, at[1])),
                out_shape=jax.ShapeDtypeStruct((n, n, wide), F32),
                input_output_aliases={} if t_i == 0 else {len(ins) - 1: 0},
                compiler_params=pltpu.CompilerParams(vmem_limit_bytes=67043328),
                name='out',
            )(*ins)
        return out

    return jax.shard_map(transform, mesh=mesh, in_specs=(P(('frag', 'dev')), P('frag')), out_specs=P('frag', None, 'dev'), check_vma=False)
```

```python
import functools

import jax
import jax.numpy as jnp
from jax import lax
from jax.experimental import pallas as pl
from jax.experimental.pallas import tpu as pltpu
from jax.sharding import PartitionSpec as P


TILES = ((0, 48, 0, 1152), (48, 24, 0, 1152), (72, 8, 0, 1152), (80, 8, 0, 1152), (88, 8, 0, 768), (88, 8, 768, 384))
PARTS = (1, 1, 1, 1, 3, 3)
DIAGONAL = (6, 7)
DIRECT = (2, 4, 3, 5, 1)
F32, BF16 = jnp.float32, jnp.bfloat16


def one_hot(shape, fn):
    rows = lax.broadcasted_iota(jnp.int32, shape, 0)
    cols = lax.broadcasted_iota(jnp.int32, shape, 1)
    return fn(rows, cols)


def dot(a, b):
    return jnp.dot(a, b, preferred_element_type=F32)


def pick(shape, fn):
    return one_hot(shape, fn).astype(BF16)


def transposed(c, n):
    eye = pick((n, n), lambda i, j: i == j)
    return lax.dot_general(c, eye, (((0,), (0,)), ((), ())), preferred_element_type=F32).astype(BF16)


def build_first(n, c_ref, l1_ref, r2_ref, ct_ref):
    c = c_ref[...]
    ct = transposed(c, n)
    ct_ref[...] = ct
    tall = dot(pick((8 * n, n), lambda i, j: i // 8 == j), ct).astype(BF16)
    wide = dot(tall, pick((n, 8 * n), lambda i, j: j % n == i))
    keep = one_hot((8 * n, 8 * n), lambda i, j: i % 8 == j // n)
    l1_ref[...] = jnp.where(keep, wide, 0.0).astype(BF16)
    tall = dot(pick((512, n), lambda i, j: i % 128 == j), c).astype(BF16)
    wide = dot(tall, pick((n, 4 * n), lambda i, j: j % n == i))
    keep = one_hot((512, 4 * n), lambda i, j: i // 128 == j // n)
    r2_ref[...] = jnp.where(keep, wide, 0.0).astype(BF16)


def last_kernel(n, rows, me_ref, c_ref, after_ref, l4_ref):
    me = me_ref[0]

    def source(r, col):
        m = col // 8
        return r == (me ^ (m // rows)) * rows + m % rows

    ct = transposed(c_ref[...], n)
    tall = dot(pick((8 * n, n), lambda i, j: i // 8 == j), ct).astype(BF16)
    wide = dot(tall, pick((n, 8 * n), source))
    keep = one_hot((8 * n, 8 * n), lambda i, j: i % 8 == j % 8)
    l4_ref[...] = jnp.where(keep, wide, 0.0).astype(BF16)


def flipped(me, k):
    out = 0
    for bit in (1, 2, 4):
        b = (me // bit) % 2
        out = out + bit * (1 - b if k & bit else b)
    return out


def exchange_kernel(n, n_dev, rows, a_hbm, c_ref, *refs):
    n_got, n_tile = n_dev - len(DIAGONAL), len(TILES)
    got, tiles = refs[:n_got], refs[n_got:n_got + len(DIAGONAL) * n_tile]
    (a_buf, t1_ref, g_ref, l1_ref, r2_ref, ct_ref, a_sem, chunk_sem, own_sem, tile_sem, send_sem,
     recv_sem) = refs[n_got + len(tiles):]
    nj = n // n_dev
    me = lax.axis_index('dev')
    barrier = pltpu.get_barrier_semaphore()
    for k in DIRECT:
        pl.semaphore_signal(barrier, inc=1, device_id={'dev': flipped(me, k)}, device_id_type=pl.DeviceIdType.MESH)

    def chunk(g):
        q = pl.ds(g * 16, 16)
        return pltpu.make_async_copy(a_hbm.at[0, q], a_buf.at[0, q], chunk_sem.at[g])

    def fetch(i):
        slot = lax.rem(i, 2)
        return pltpu.make_async_copy(a_hbm.at[i], a_buf.at[slot], a_sem.at[slot])

    for g in range(n // 16):
        chunk(g).start()
    fetch(1).start()
    build_first(n, c_ref, l1_ref, r2_ref, ct_ref)
    zero = jnp.zeros((8 * n, 128 - n), BF16)

    def remote(k, src, dst):
        return pltpu.make_async_remote_copy(
            src_ref=src, dst_ref=dst, send_sem=send_sem.at[k], recv_sem=recv_sem.at[k],
            device_id={'dev': flipped(me, k)}, device_id_type=pl.DeviceIdType.MESH)

    def tile_copies(k, rows_):
        x = DIAGONAL.index(k)
        for t, (a0, size, lane, lanes) in enumerate(TILES):
            j = x * n_tile + t
            src = g_ref.at[k, rows_, pl.ds(a0, size), pl.ds(lane, lanes)]
            yield pltpu.make_async_copy(src, tiles[j].at[rows_], tile_sem.at[j])

    def send(k, i):
        if k == 0:
            pltpu.make_async_copy(g_ref.at[0, i], got[0].at[i], own_sem).start()
        elif k in DIAGONAL:
            for copy in tile_copies(k, i):
                copy.start()
        else:
            remote(k, g_ref.at[k, i], got[k].at[i]).start()

    def step_one(slot, g, lhs):
        q0 = pl.multiple_of(g * 16, 16)
        lo = a_buf[slot, pl.ds(q0, 8)].reshape(8 * n, n)
        hi = a_buf[slot, pl.ds(q0 + 8, 8)].reshape(8 * n, n)
        t = dot(lhs, jnp.concatenate([lo, zero, hi, zero], axis=1))
        nj = t.shape[0] // 8
        t = jnp.concatenate([t[:, :128].reshape(nj, 8, 128), t[:, 128:].reshape(nj, 8, 128)], axis=1)
        return pl.ds(q0, 16), t.astype(BF16)

    def step_two_three(k, i):
        d = flipped(me, k)
        t = t1_ref[pl.ds(d * nj, nj)].reshape(nj // 4, 4, n, 128)
        lhs = jnp.concatenate([t[:, jj].reshape(nj // 4 * n, 128) for jj in range(4)], axis=1)
        h = dot(lhs, r2_ref[...]).astype(BF16)
        h = jnp.concatenate([h[g * n:(g + 1) * n] for g in range(nj // 4)], axis=1)
        g_ref[k, i] = dot(ct_ref[...], h).astype(BF16)

    def some(ks, i, slot, wait):
        def first(g, carry):
            if wait:
                chunk(g).wait()
            lhs = jnp.concatenate(
                [l1_ref[pl.ds(pl.multiple_of(flipped(me, k) * 8 * nj, 8 * nj), 8 * nj)] for k in ks], axis=0)
            q, t = step_one(slot, g, lhs)
            for x, k in enumerate(ks):
                t1_ref[pl.ds(flipped(me, k) * nj, nj), q, :] = t[x * nj:(x + 1) * nj]
            return carry

        lax.fori_loop(0, n // 16, first, 0)
        before = None
        for k in ks:
            step_two_three(k, i)
            if before is not None:
                send(before, i)
            elif wait:
                pl.semaphore_wait(barrier, len(DIRECT))
            before = k
        send(before, i)

    some(DIRECT[:2], 0, 0, True)
    some((*DIRECT[2:], 0, *DIAGONAL), 0, 0, False)

    def row(i, carry):
        slot = lax.rem(i, 2)
        fetch(i).wait()

        @pl.when(i + 1 < rows)
        def _():
            fetch(i + 1).start()

        def first(g, carry):
            q, t = step_one(slot, g, l1_ref[...])
            t1_ref[:, q, :] = t
            return carry

        lax.fori_loop(0, n // 16, first, 0)
        before = None
        for k in (*DIRECT, 0, *DIAGONAL):
            step_two_three(k, i)
            if before is not None:
                send(before, i)
            before = k
        send(before, i)
        return carry

    lax.fori_loop(1, rows, row, 0)
    pltpu.make_async_copy(g_ref.at[0], got[0], own_sem).wait()
    for k in DIAGONAL:
        for copy in tile_copies(k, pl.ds(0, rows)):
            copy.wait()
    for k in DIRECT:
        remote(k, g_ref.at[k], got[k]).wait()


def out_kernel(n_in, wide, *refs):
    l4_ref, out_ref = refs[n_in], refs[-1]
    rhs = jnp.concatenate([r[...].reshape(-1, wide) for r in refs[:n_in]], axis=0)
    out_ref[...] = dot(l4_ref[...], rhs).reshape(out_ref.shape)


def solution(mesh):
    n_dev = mesh.shape['dev']

    def transform(ao_rows, coeffs):
        rows = ao_rows.shape[0]
        n = coeffs.shape[0]
        wide = n * n // n_dev
        me_arr = jnp.full((1,), lax.axis_index('dev'), jnp.int32)
        smem = pl.BlockSpec(memory_space=pltpu.SMEM)
        vmem = pl.BlockSpec(memory_space=pltpu.VMEM)
        hbm = pl.BlockSpec(memory_space=pl.ANY)

        square, second = (8 * n, 8 * n), (512, 4 * n)
        n_got = n_dev - len(DIAGONAL)
        shapes = [(rows, n, wide)] * n_got
        shapes += [(rows, size, lanes) for _ in DIAGONAL for _, size, _, lanes in TILES]
        outs = pl.pallas_call(
            functools.partial(exchange_kernel, n, n_dev, rows),
            in_specs=[hbm, vmem],
            out_specs=[hbm] * len(shapes),
            out_shape=[jax.ShapeDtypeStruct(s, BF16) for s in shapes],
            scratch_shapes=[
                pltpu.VMEM((2, n, n, n), BF16), pltpu.VMEM((n, n, 128), BF16),
                pltpu.VMEM((n_dev, rows, n, wide), BF16), pltpu.VMEM(square, BF16),
                pltpu.VMEM(second, BF16), pltpu.VMEM((n, n), BF16),
                pltpu.SemaphoreType.DMA((2,)), pltpu.SemaphoreType.DMA((n // 16,)), pltpu.SemaphoreType.DMA,
                pltpu.SemaphoreType.DMA((len(shapes) - n_got,)),
                pltpu.SemaphoreType.DMA((n_dev,)), pltpu.SemaphoreType.DMA((n_dev,))],
            compiler_params=pltpu.CompilerParams(collective_id=0, has_side_effects=True),
            name='exchange',
        )(ao_rows, coeffs)
        got, tiles = outs[:n_got], outs[n_got:]
        moved = {}
        for t in range(len(TILES)):
            for x, k in enumerate(DIAGONAL):
                moved[k, t] = lax.ppermute(
                    tiles[x * len(TILES) + t], 'dev', [(i, i ^ k) for i in range(n_dev)])
        l4 = pl.pallas_call(
            functools.partial(last_kernel, n, rows),
            in_specs=[smem, vmem, hbm],
            out_specs=vmem,
            out_shape=jax.ShapeDtypeStruct(square, BF16),
            name='last',
        )(me_arr, coeffs, got[0])

        out = None
        for t_i, (a0, size, lane, lanes) in enumerate(TILES):
            ins, specs = [], []
            for k in range(n_dev):
                block, at = (moved[k, t_i], (0, 0)) if (k, t_i) in moved else (got[k], (a0 // 8, lane // lanes))
                ins.append(block)
                specs.append(pl.BlockSpec((rows, 8, lanes), lambda i, j, at=at: (0, at[0] + i, at[1])))
            n_in = len(ins)
            ins.append(l4)
            parts = PARTS[t_i]
            specs.append(pl.BlockSpec((8 * n // parts, 8 * n), lambda i, j: (j, 0)))
            if out is not None:
                ins.append(out)
                specs.append(hbm)
            out = pl.pallas_call(
                functools.partial(out_kernel, n_in, lanes),
                grid=(size // 8, parts),
                in_specs=specs,
                out_specs=pl.BlockSpec((n // parts, 8, lanes), lambda i, j, at=(a0 // 8, lane // lanes): (j, at[0] + i, at[1])),
                out_shape=jax.ShapeDtypeStruct((n, n, wide), F32),
                input_output_aliases={} if t_i == 0 else {len(ins) - 1: 0},
                compiler_params=pltpu.CompilerParams(vmem_limit_bytes=67043328),
                name='out',
            )(*ins)
        return out

    return jax.shard_map(transform, mesh=mesh, in_specs=(P(('frag', 'dev')), P('frag')), out_specs=P('frag', None, 'dev'), check_vma=False)
```

```python
import functools

import jax
import jax.numpy as jnp
from jax import lax
from jax.experimental import pallas as pl
from jax.experimental.pallas import tpu as pltpu
from jax.sharding import PartitionSpec as P


TILES = ((0, 48, 0, 1152), (48, 24, 0, 1152), (72, 8, 0, 1152), (80, 8, 0, 1152), (88, 8, 0, 640), (88, 8, 640, 512))
DIAGONAL = (6, 7)
DIRECT = (2, 4, 3, 5, 1)
F32, BF16 = jnp.float32, jnp.bfloat16


def one_hot(shape, fn):
    rows = lax.broadcasted_iota(jnp.int32, shape, 0)
    cols = lax.broadcasted_iota(jnp.int32, shape, 1)
    return fn(rows, cols)


def dot(a, b):
    return jnp.dot(a, b, preferred_element_type=F32)


def pick(shape, fn):
    return one_hot(shape, fn).astype(BF16)


def transposed(c, n):
    eye = pick((n, n), lambda i, j: i == j)
    return lax.dot_general(c, eye, (((0,), (0,)), ((), ())), preferred_element_type=F32).astype(BF16)


def build_first(n, c_ref, l1_ref, r2_ref, ct_ref):
    c = c_ref[...]
    ct = transposed(c, n)
    ct_ref[...] = ct
    tall = dot(pick((8 * n, n), lambda i, j: i // 8 == j), ct).astype(BF16)
    wide = dot(tall, pick((n, 8 * n), lambda i, j: j % n == i))
    keep = one_hot((8 * n, 8 * n), lambda i, j: i % 8 == j // n)
    l1_ref[...] = jnp.where(keep, wide, 0.0).astype(BF16)
    tall = dot(pick((512, n), lambda i, j: i % 128 == j), c).astype(BF16)
    wide = dot(tall, pick((n, 4 * n), lambda i, j: j % n == i))
    keep = one_hot((512, 4 * n), lambda i, j: i // 128 == j // n)
    r2_ref[...] = jnp.where(keep, wide, 0.0).astype(BF16)


def last_kernel(n, rows, me_ref, c_ref, after_ref, l4_ref):
    me = me_ref[0]

    def source(r, col):
        m = col // 8
        return r == (me ^ (m // rows)) * rows + m % rows

    ct = transposed(c_ref[...], n)
    tall = dot(pick((8 * n, n), lambda i, j: i // 8 == j), ct).astype(BF16)
    wide = dot(tall, pick((n, 8 * n), source))
    keep = one_hot((8 * n, 8 * n), lambda i, j: i % 8 == j % 8)
    l4_ref[...] = jnp.where(keep, wide, 0.0).astype(BF16)


def flipped(me, k):
    out = 0
    for bit in (1, 2, 4):
        b = (me // bit) % 2
        out = out + bit * (1 - b if k & bit else b)
    return out


def exchange_kernel(n, n_dev, rows, a_hbm, c_ref, *refs):
    n_got, n_tile = n_dev - len(DIAGONAL), len(TILES)
    got, tiles = refs[:n_got], refs[n_got:n_got + len(DIAGONAL) * n_tile]
    (a_buf, t1_ref, g_ref, l1_ref, r2_ref, ct_ref, a_sem, chunk_sem, own_sem, tile_sem, send_sem,
     recv_sem) = refs[n_got + len(tiles):]
    nj = n // n_dev
    me = lax.axis_index('dev')
    barrier = pltpu.get_barrier_semaphore()
    for k in DIRECT:
        pl.semaphore_signal(barrier, inc=1, device_id={'dev': flipped(me, k)}, device_id_type=pl.DeviceIdType.MESH)

    def chunk(g):
        q = pl.ds(g * 16, 16)
        return pltpu.make_async_copy(a_hbm.at[0, q], a_buf.at[0, q], chunk_sem.at[g])

    def fetch(i):
        slot = lax.rem(i, 2)
        return pltpu.make_async_copy(a_hbm.at[i], a_buf.at[slot], a_sem.at[slot])

    for g in range(n // 16):
        chunk(g).start()
    fetch(1).start()
    build_first(n, c_ref, l1_ref, r2_ref, ct_ref)
    zero = jnp.zeros((8 * n, 128 - n), BF16)

    def remote(k, src, dst):
        return pltpu.make_async_remote_copy(
            src_ref=src, dst_ref=dst, send_sem=send_sem.at[k], recv_sem=recv_sem.at[k],
            device_id={'dev': flipped(me, k)}, device_id_type=pl.DeviceIdType.MESH)

    def tile_copies(k, rows_):
        x = DIAGONAL.index(k)
        for t, (a0, size, lane, lanes) in enumerate(TILES):
            j = x * n_tile + t
            src = g_ref.at[k, rows_, pl.ds(a0, size), pl.ds(lane, lanes)]
            yield pltpu.make_async_copy(src, tiles[j].at[rows_], tile_sem.at[j])

    def send(k, i):
        if k == 0:
            pltpu.make_async_copy(g_ref.at[0, i], got[0].at[i], own_sem).start()
        elif k in DIAGONAL:
            for copy in tile_copies(k, i):
                copy.start()
        else:
            remote(k, g_ref.at[k, i], got[k].at[i]).start()

    def step_one(slot, g, lhs):
        q0 = pl.multiple_of(g * 16, 16)
        lo = a_buf[slot, pl.ds(q0, 8)].reshape(8 * n, n)
        hi = a_buf[slot, pl.ds(q0 + 8, 8)].reshape(8 * n, n)
        t = dot(lhs, jnp.concatenate([lo, zero, hi, zero], axis=1))
        nj = t.shape[0] // 8
        t = jnp.concatenate([t[:, :128].reshape(nj, 8, 128), t[:, 128:].reshape(nj, 8, 128)], axis=1)
        return pl.ds(q0, 16), t.astype(BF16)

    def step_two_three(k, i):
        d = flipped(me, k)
        t = t1_ref[pl.ds(d * nj, nj)].reshape(nj // 4, 4, n, 128)
        lhs = jnp.concatenate([t[:, jj].reshape(nj // 4 * n, 128) for jj in range(4)], axis=1)
        h = dot(lhs, r2_ref[...]).astype(BF16)
        h = jnp.concatenate([h[g * n:(g + 1) * n] for g in range(nj // 4)], axis=1)
        g_ref[k, i] = dot(ct_ref[...], h).astype(BF16)

    def some(ks, i, slot, wait):
        def first(g, carry):
            if wait:
                chunk(g).wait()
            lhs = jnp.concatenate(
                [l1_ref[pl.ds(pl.multiple_of(flipped(me, k) * 8 * nj, 8 * nj), 8 * nj)] for k in ks], axis=0)
            q, t = step_one(slot, g, lhs)
            for x, k in enumerate(ks):
                t1_ref[pl.ds(flipped(me, k) * nj, nj), q, :] = t[x * nj:(x + 1) * nj]
            return carry

        lax.fori_loop(0, n // 16, first, 0)
        before = None
        for k in ks:
            step_two_three(k, i)
            if before is not None:
                send(before, i)
            elif wait:
                pl.semaphore_wait(barrier, len(DIRECT))
            before = k
        send(before, i)

    some(DIRECT[:2], 0, 0, True)
    some((*DIRECT[2:], 0, *DIAGONAL), 0, 0, False)

    def row(i, carry):
        slot = lax.rem(i, 2)
        fetch(i).wait()

        @pl.when(i + 1 < rows)
        def _():
            fetch(i + 1).start()

        def first(g, carry):
            q, t = step_one(slot, g, l1_ref[...])
            t1_ref[:, q, :] = t
            return carry

        lax.fori_loop(0, n // 16, first, 0)
        before = None
        for k in (*DIRECT, 0, *DIAGONAL):
            step_two_three(k, i)
            if before is not None:
                send(before, i)
            before = k
        send(before, i)
        return carry

    lax.fori_loop(1, rows, row, 0)
    pltpu.make_async_copy(g_ref.at[0], got[0], own_sem).wait()
    for k in DIAGONAL:
        for copy in tile_copies(k, pl.ds(0, rows)):
            copy.wait()
    for k in DIRECT:
        remote(k, g_ref.at[k], got[k]).wait()


def out_kernel(n_in, wide, *refs):
    l4_ref, out_ref = refs[n_in], refs[-1]
    rhs = jnp.concatenate([r[...].reshape(-1, wide) for r in refs[:n_in]], axis=0)
    out_ref[...] = dot(l4_ref[...], rhs).reshape(out_ref.shape)


def tail_kernel(n, n_in, a0, lane, lanes, parts, *refs):
    l4_ref, out_hbm, (v_ref, sem) = refs[n_in], refs[-3], refs[-2:]
    rhs = jnp.concatenate([r[...].reshape(-1, lanes) for r in refs[:n_in]], axis=0)
    size = n // parts
    copies = []
    for x in range(parts):
        i = pl.ds(x * size, size)
        v_ref[i] = dot(l4_ref[pl.ds(8 * size * x, 8 * size)], rhs).reshape(size, 8, lanes)
        copies.append(pltpu.make_async_copy(
            v_ref.at[i], out_hbm.at[i, pl.ds(a0, 8), pl.ds(lane, lanes)], sem.at[x]))
        copies[-1].start()
    for copy in copies:
        copy.wait()


def solution(mesh):
    n_dev = mesh.shape['dev']

    def transform(ao_rows, coeffs):
        rows = ao_rows.shape[0]
        n = coeffs.shape[0]
        wide = n * n // n_dev
        me_arr = jnp.full((1,), lax.axis_index('dev'), jnp.int32)
        smem = pl.BlockSpec(memory_space=pltpu.SMEM)
        vmem = pl.BlockSpec(memory_space=pltpu.VMEM)
        hbm = pl.BlockSpec(memory_space=pl.ANY)

        def const(shape):
            return pl.BlockSpec(shape, lambda *_: (0,) * len(shape))

        square, second = (8 * n, 8 * n), (512, 4 * n)
        n_got = n_dev - len(DIAGONAL)
        shapes = [(rows, n, wide)] * n_got
        shapes += [(rows, size, lanes) for _ in DIAGONAL for _, size, _, lanes in TILES]
        outs = pl.pallas_call(
            functools.partial(exchange_kernel, n, n_dev, rows),
            in_specs=[hbm, vmem],
            out_specs=[hbm] * len(shapes),
            out_shape=[jax.ShapeDtypeStruct(s, BF16) for s in shapes],
            scratch_shapes=[
                pltpu.VMEM((2, n, n, n), BF16), pltpu.VMEM((n, n, 128), BF16),
                pltpu.VMEM((n_dev, rows, n, wide), BF16), pltpu.VMEM(square, BF16),
                pltpu.VMEM(second, BF16), pltpu.VMEM((n, n), BF16),
                pltpu.SemaphoreType.DMA((2,)), pltpu.SemaphoreType.DMA((n // 16,)), pltpu.SemaphoreType.DMA,
                pltpu.SemaphoreType.DMA((len(shapes) - n_got,)),
                pltpu.SemaphoreType.DMA((n_dev,)), pltpu.SemaphoreType.DMA((n_dev,))],
            compiler_params=pltpu.CompilerParams(collective_id=0, has_side_effects=True),
            name='exchange',
        )(ao_rows, coeffs)
        got, tiles = outs[:n_got], outs[n_got:]
        moved = {}
        for t in range(len(TILES)):
            for x, k in enumerate(DIAGONAL):
                moved[k, t] = lax.ppermute(
                    tiles[x * len(TILES) + t], 'dev', [(i, i ^ k) for i in range(n_dev)])
        l4 = pl.pallas_call(
            functools.partial(last_kernel, n, rows),
            in_specs=[smem, vmem, hbm],
            out_specs=vmem,
            out_shape=jax.ShapeDtypeStruct(square, BF16),
            name='last',
        )(me_arr, coeffs, got[0])

        out = None
        for t_i, (a0, size, lane, lanes) in enumerate(TILES):
            ins, specs = [], []
            for k in range(n_dev):
                block, at = (moved[k, t_i], (0, 0)) if (k, t_i) in moved else (got[k], (a0, lane))
                ins.append(block)
                specs.append(pl.BlockSpec((pl.Element(rows), pl.Element(8), pl.Element(lanes)), lambda i, at=at: (0, pl.multiple_of(at[0] + 8 * i, 8), at[1])))
            n_in = len(ins)
            ins.append(l4)
            specs.append(const(square))
            if out is not None:
                ins.append(out)
                specs.append(hbm)
            alone = size == 8
            out = pl.pallas_call(
                functools.partial(tail_kernel, n, n_in, a0, lane, lanes, 3) if alone
                else functools.partial(out_kernel, n_in, lanes),
                grid=(size // 8,),
                in_specs=specs,
                out_specs=hbm if alone else pl.BlockSpec(
                    (pl.Element(n), pl.Element(8), pl.Element(lanes)),
                    lambda i, at=(a0, lane): (0, pl.multiple_of(at[0] + 8 * i, 8), at[1])),
                out_shape=jax.ShapeDtypeStruct((n, n, wide), F32),
                input_output_aliases={} if t_i == 0 else {len(ins) - 1: 0},
                scratch_shapes=[pltpu.VMEM((n, 8, lanes), F32), pltpu.SemaphoreType.DMA((3,))] * alone,
                compiler_params=pltpu.CompilerParams(vmem_limit_bytes=67043328),
                name='out',
            )(*ins)
        return out

    return jax.shard_map(transform, mesh=mesh, in_specs=(P(('frag', 'dev')), P('frag')), out_specs=P('frag', None, 'dev'), check_vma=False)
```

```python
import functools

import jax
import jax.numpy as jnp
from jax import lax
from jax.experimental import pallas as pl
from jax.experimental.pallas import tpu as pltpu
from jax.sharding import PartitionSpec as P


TILES = ((0, 48, 0, 1152), (48, 24, 0, 1152), (72, 8, 0, 1152), (80, 8, 0, 1152), (88, 8, 0, 768), (88, 8, 768, 384))
TAIL = 88
DIAGONAL = (6, 7)
DIRECT = (2, 4, 3, 5, 1)
F32, BF16 = jnp.float32, jnp.bfloat16


def one_hot(shape, fn):
    rows = lax.broadcasted_iota(jnp.int32, shape, 0)
    cols = lax.broadcasted_iota(jnp.int32, shape, 1)
    return fn(rows, cols)


def dot(a, b):
    return jnp.dot(a, b, preferred_element_type=F32)


def pick(shape, fn):
    return one_hot(shape, fn).astype(BF16)


def transposed(c, n):
    eye = pick((n, n), lambda i, j: i == j)
    return lax.dot_general(c, eye, (((0,), (0,)), ((), ())), preferred_element_type=F32).astype(BF16)


def build_small(n, c_ref, r2_ref, ct_ref):
    c = c_ref[...]
    ct_ref[...] = transposed(c, n)
    tall = dot(pick((512, n), lambda i, j: i % 128 == j), c).astype(BF16)
    wide = dot(tall, pick((n, 4 * n), lambda i, j: j % n == i))
    keep = one_hot((512, 4 * n), lambda i, j: i // 128 == j // n)
    r2_ref[...] = jnp.where(keep, wide, 0.0).astype(BF16)


def build_l1(n, first, size, ct_ref, l1_ref):
    tall = dot(pick((8 * size, n), lambda i, j: i // 8 + first == j), ct_ref[...]).astype(BF16)
    wide = dot(tall, pick((n, 8 * n), lambda i, j: j % n == i))
    keep = one_hot((8 * size, 8 * n), lambda i, j: i % 8 == j // n)
    l1_ref[pl.ds(pl.multiple_of(first * 8, 8 * size), 8 * size)] = jnp.where(keep, wide, 0.0).astype(BF16)


def last_kernel(n, rows, spans, me_ref, c_ref, after_ref, *l4_refs):
    me = me_ref[0]
    ct = transposed(c_ref[...], n)
    tall = dot(pick((8 * n, n), lambda i, j: i // 8 == j), ct).astype(BF16)
    for (k0, k1), l4_ref in zip(spans, l4_refs):
        def source(r, col, k0=k0):
            m = col // 8 + k0 * rows
            return r == (me ^ (m // rows)) * rows + m % rows

        width = 8 * rows * (k1 - k0)
        wide = dot(tall, pick((n, width), source))
        keep = one_hot((8 * n, width), lambda i, j: i % 8 == j % 8)
        l4_ref[...] = jnp.where(keep, wide, 0.0).astype(BF16)


def flipped(me, k):
    out = 0
    for bit in (1, 2, 4):
        b = (me // bit) % 2
        out = out + bit * (1 - b if k & bit else b)
    return out


def exchange_kernel(n, n_dev, rows, a_hbm, c_ref, *refs):
    n_got, n_tile = n_dev - len(DIAGONAL), len(TILES)
    got, tiles = refs[:n_got], refs[n_got:n_got + len(DIAGONAL) * n_tile]
    (a_buf, t1_ref, g_ref, l1_ref, r2_ref, ct_ref, a_sem, chunk_sem, own_sem, tile_sem, send_sem,
     recv_sem) = refs[n_got + len(tiles):]
    nj = n // n_dev
    me = lax.axis_index('dev')
    barrier = pltpu.get_barrier_semaphore()
    for k in DIRECT:
        pl.semaphore_signal(barrier, inc=1, device_id={'dev': flipped(me, k)}, device_id_type=pl.DeviceIdType.MESH)

    def chunk(g):
        q = pl.ds(g * 16, 16)
        return pltpu.make_async_copy(a_hbm.at[0, q], a_buf.at[0, q], chunk_sem.at[g])

    def fetch(i):
        slot = lax.rem(i, 2)
        return pltpu.make_async_copy(a_hbm.at[i], a_buf.at[slot], a_sem.at[slot])

    for g in range(n // 16):
        chunk(g).start()
    fetch(1).start()
    build_small(n, c_ref, r2_ref, ct_ref)
    for k in DIRECT[:2]:
        build_l1(n, flipped(me, k) * nj, nj, ct_ref, l1_ref)
    zero = jnp.zeros((8 * n, 128 - n), BF16)

    def remote(k, src, dst):
        return pltpu.make_async_remote_copy(
            src_ref=src, dst_ref=dst, send_sem=send_sem.at[k], recv_sem=recv_sem.at[k],
            device_id={'dev': flipped(me, k)}, device_id_type=pl.DeviceIdType.MESH)

    def tile_copies(k, rows_):
        x = DIAGONAL.index(k)
        for t, (a0, size, lane, lanes) in enumerate(TILES):
            j = x * n_tile + t
            src = g_ref.at[k, rows_, pl.ds(a0, size), pl.ds(lane, lanes)]
            yield pltpu.make_async_copy(src, tiles[j].at[rows_], tile_sem.at[j])

    def send(k, i):
        if k == 0:
            pltpu.make_async_copy(g_ref.at[0, i], got[0].at[i], own_sem).start()
        elif k in DIAGONAL:
            for copy in tile_copies(k, i):
                copy.start()
        else:
            remote(k, g_ref.at[k, i], got[k].at[i]).start()

    def step_one(slot, g, lhs):
        q0 = pl.multiple_of(g * 16, 16)
        lo = a_buf[slot, pl.ds(q0, 8)].reshape(8 * n, n)
        hi = a_buf[slot, pl.ds(q0 + 8, 8)].reshape(8 * n, n)
        t = dot(lhs, jnp.concatenate([lo, zero, hi, zero], axis=1))
        nj = t.shape[0] // 8
        t = jnp.concatenate([t[:, :128].reshape(nj, 8, 128), t[:, 128:].reshape(nj, 8, 128)], axis=1)
        return pl.ds(q0, 16), t.astype(BF16)

    def step_two_three(k, i):
        d = flipped(me, k)
        t = t1_ref[pl.ds(d * nj, nj)].reshape(nj // 4, 4, n, 128)
        lhs = jnp.concatenate([t[:, jj].reshape(nj // 4 * n, 128) for jj in range(4)], axis=1)
        h = dot(lhs, r2_ref[...]).astype(BF16)
        h = jnp.concatenate([h[g * n:(g + 1) * n] for g in range(nj // 4)], axis=1)
        g_ref[k, i] = dot(ct_ref[...], h).astype(BF16)

    def some(ks, i, slot, wait):
        def first(g, carry):
            if wait:
                chunk(g).wait()
            lhs = jnp.concatenate(
                [l1_ref[pl.ds(pl.multiple_of(flipped(me, k) * 8 * nj, 8 * nj), 8 * nj)] for k in ks], axis=0)
            q, t = step_one(slot, g, lhs)
            for x, k in enumerate(ks):
                t1_ref[pl.ds(flipped(me, k) * nj, nj), q, :] = t[x * nj:(x + 1) * nj]
            return carry

        lax.fori_loop(0, n // 16, first, 0)
        before = None
        for k in ks:
            step_two_three(k, i)
            if before is not None:
                send(before, i)
            elif wait:
                pl.semaphore_wait(barrier, len(DIRECT))
            before = k
        send(before, i)

    some(DIRECT[:2], 0, 0, True)
    build_l1(n, 0, n, ct_ref, l1_ref)
    some((*DIRECT[2:], 0, *DIAGONAL), 0, 0, False)

    def row(i, carry):
        slot = lax.rem(i, 2)
        fetch(i).wait()

        @pl.when(i + 1 < rows)
        def _():
            fetch(i + 1).start()

        def first(g, carry):
            q, t = step_one(slot, g, l1_ref[...])
            t1_ref[:, q, :] = t
            return carry

        lax.fori_loop(0, n // 16, first, 0)
        before = None
        for k in (*DIRECT, 0, *DIAGONAL):
            step_two_three(k, i)
            if before is not None:
                send(before, i)
            before = k
        send(before, i)
        return carry

    lax.fori_loop(1, rows, row, 0)
    pltpu.make_async_copy(g_ref.at[0], got[0], own_sem).wait()
    for k in DIAGONAL:
        for copy in tile_copies(k, pl.ds(0, rows)):
            copy.wait()
    for k in DIRECT:
        remote(k, g_ref.at[k], got[k]).wait()


def out_kernel(n_in, wide, *refs):
    l4_ref, out_ref = refs[n_in], refs[-1]
    rhs = jnp.concatenate([r[...].reshape(-1, wide) for r in refs[:n_in]], axis=0)
    out_ref[...] = dot(l4_ref[...], rhs).reshape(out_ref.shape)


def tail_kernel(n, n_in, a0, lane, lanes, parts, *refs):
    l4_ref, v_hbm, out_hbm, v_ref, in_sem, out_sem = refs[n_in:]
    size = n // parts

    def part(x):
        return pl.ds(x * size, size), pl.ds(a0, 8), pl.ds(lane, lanes)

    loads = [pltpu.make_async_copy(v_hbm.at[part(x)], v_ref.at[part(x)[0]], in_sem.at[x]) for x in range(parts)]
    for copy in loads:
        copy.start()
    rhs = jnp.concatenate([r[...].reshape(-1, lanes) for r in refs[:n_in]], axis=0)
    copies = []
    for x in range(parts):
        i = part(x)[0]
        v = dot(l4_ref[pl.ds(8 * size * x, 8 * size)], rhs).reshape(size, 8, lanes)
        loads[x].wait()
        v_ref[i] = v_ref[i] + v
        copies.append(pltpu.make_async_copy(v_ref.at[i], out_hbm.at[part(x)], out_sem.at[x]))
        copies[-1].start()
    for copy in copies:
        copy.wait()


def solution(mesh):
    n_dev = mesh.shape['dev']

    def transform(ao_rows, coeffs):
        rows = ao_rows.shape[0]
        n = coeffs.shape[0]
        wide = n * n // n_dev
        me_arr = jnp.full((1,), lax.axis_index('dev'), jnp.int32)
        smem = pl.BlockSpec(memory_space=pltpu.SMEM)
        vmem = pl.BlockSpec(memory_space=pltpu.VMEM)
        hbm = pl.BlockSpec(memory_space=pl.ANY)

        def const(shape):
            return pl.BlockSpec(shape, lambda *_: (0,) * len(shape))

        square, second = (8 * n, 8 * n), (512, 4 * n)
        n_got = n_dev - len(DIAGONAL)
        shapes = [(rows, n, wide)] * n_got
        shapes += [(rows, size, lanes) for _ in DIAGONAL for _, size, _, lanes in TILES]
        outs = pl.pallas_call(
            functools.partial(exchange_kernel, n, n_dev, rows),
            in_specs=[hbm, vmem],
            out_specs=[hbm] * len(shapes),
            out_shape=[jax.ShapeDtypeStruct(s, BF16) for s in shapes],
            scratch_shapes=[
                pltpu.VMEM((2, n, n, n), BF16), pltpu.VMEM((n, n, 128), BF16),
                pltpu.VMEM((n_dev, rows, n, wide), BF16), pltpu.VMEM(square, BF16),
                pltpu.VMEM(second, BF16), pltpu.VMEM((n, n), BF16),
                pltpu.SemaphoreType.DMA((2,)), pltpu.SemaphoreType.DMA((n // 16,)), pltpu.SemaphoreType.DMA,
                pltpu.SemaphoreType.DMA((len(shapes) - n_got,)),
                pltpu.SemaphoreType.DMA((n_dev,)), pltpu.SemaphoreType.DMA((n_dev,))],
            compiler_params=pltpu.CompilerParams(collective_id=0, has_side_effects=True),
            name='exchange',
        )(ao_rows, coeffs)
        got, tiles = outs[:n_got], outs[n_got:]
        moved = {}
        for t in range(len(TILES)):
            for x, k in enumerate(DIAGONAL):
                moved[k, t] = lax.ppermute(
                    tiles[x * len(TILES) + t], 'dev', [(i, i ^ k) for i in range(n_dev)])
        spans = ((0, n_dev), (0, n_got), (n_got, n_dev))
        widths = [8 * rows * (k1 - k0) for k0, k1 in spans]
        l4, l4_direct, l4_diagonal = pl.pallas_call(
            functools.partial(last_kernel, n, rows, spans),
            in_specs=[smem, vmem, hbm],
            out_specs=[vmem] * 3,
            out_shape=[jax.ShapeDtypeStruct((8 * n, w), BF16) for w in widths],
            name='last',
        )(me_arr, coeffs, got[0])

        def spec(size, a0, lane, lanes):
            return pl.BlockSpec(tuple(map(pl.Element, (size, 8, lanes))),
                                lambda i: (0, pl.multiple_of(a0 + 8 * i, 8), lane))

        parts = 3
        out = None
        for t_i, (a0, size, lane, lanes) in ((None, (TAIL, n - TAIL, 0, wide)), *enumerate(TILES)):
            ins, specs = [], []
            for k in range(n_dev):
                if (k, t_i) in moved:
                    ins.append(moved[k, t_i])
                    specs.append(spec(rows, 0, 0, lanes))
                elif k < n_got and (t_i is None or a0 < TAIL):
                    ins.append(got[k])
                    specs.append(spec(rows, a0, lane, lanes))
            n_in = len(ins)
            tail = t_i is not None and a0 >= TAIL
            ins.append(l4_direct if t_i is None else l4_diagonal if tail else l4)
            specs.append(const(ins[-1].shape))
            if out is not None:
                ins.append(out)
                specs.append(hbm)
            out = pl.pallas_call(
                functools.partial(tail_kernel, n, n_in, a0, lane, lanes, parts) if tail
                else functools.partial(out_kernel, n_in, lanes),
                grid=(size // 8,),
                in_specs=specs,
                out_specs=hbm if tail else spec(n, a0, lane, lanes),
                out_shape=jax.ShapeDtypeStruct((n, n, wide), F32),
                input_output_aliases={} if t_i is None else {len(ins) - 1: 0},
                scratch_shapes=[pltpu.VMEM((n, 8, lanes), F32), pltpu.SemaphoreType.DMA((parts,)),
                                pltpu.SemaphoreType.DMA((parts,))] * tail,
                compiler_params=pltpu.CompilerParams(vmem_limit_bytes=67043328),
                name='out',
            )(*ins)
        return out

    return jax.shard_map(transform, mesh=mesh, in_specs=(P(('frag', 'dev')), P('frag')), out_specs=P('frag', None, 'dev'), check_vma=False)
```

```python
import functools

import jax
import jax.numpy as jnp
from jax import lax
from jax.experimental import pallas as pl
from jax.experimental.pallas import tpu as pltpu
from jax.sharding import PartitionSpec as P


TILES = ((0, 48, 0, 1152), (48, 24, 0, 1152), (72, 8, 0, 1152), (80, 8, 0, 1152), (88, 8, 0, 640), (88, 8, 640, 512))
DIAGONAL = (6, 7)
DIRECT = (2, 4, 3, 5, 1)
F32, BF16 = jnp.float32, jnp.bfloat16


def one_hot(shape, fn):
    rows = lax.broadcasted_iota(jnp.int32, shape, 0)
    cols = lax.broadcasted_iota(jnp.int32, shape, 1)
    return fn(rows, cols)


def dot(a, b):
    return jnp.dot(a, b, preferred_element_type=F32)


def pick(shape, fn):
    return one_hot(shape, fn).astype(BF16)


def transposed(c, n):
    eye = pick((n, n), lambda i, j: i == j)
    return lax.dot_general(c, eye, (((0,), (0,)), ((), ())), preferred_element_type=F32).astype(BF16)


def build_small(n, c_ref, r2_ref, ct_ref):
    c = c_ref[...]
    ct_ref[...] = transposed(c, n)
    tall = dot(pick((512, n), lambda i, j: i % 128 == j), c).astype(BF16)
    wide = dot(tall, pick((n, 4 * n), lambda i, j: j % n == i))
    keep = one_hot((512, 4 * n), lambda i, j: i // 128 == j // n)
    r2_ref[...] = jnp.where(keep, wide, 0.0).astype(BF16)


def build_l1(n, first, size, ct_ref, l1_ref):
    tall = dot(pick((8 * size, n), lambda i, j: i // 8 + first == j), ct_ref[...]).astype(BF16)
    wide = dot(tall, pick((n, 8 * n), lambda i, j: j % n == i))
    keep = one_hot((8 * size, 8 * n), lambda i, j: i % 8 == j // n)
    l1_ref[pl.ds(pl.multiple_of(first * 8, 8 * size), 8 * size)] = jnp.where(keep, wide, 0.0).astype(BF16)


def last_kernel(n, rows, me_ref, c_ref, after_ref, l4_ref):
    me = me_ref[0]

    def source(r, col):
        m = col // 8
        return r == (me ^ (m // rows)) * rows + m % rows

    ct = transposed(c_ref[...], n)
    tall = dot(pick((8 * n, n), lambda i, j: i // 8 == j), ct).astype(BF16)
    wide = dot(tall, pick((n, 8 * n), source))
    keep = one_hot((8 * n, 8 * n), lambda i, j: i % 8 == j % 8)
    l4_ref[...] = jnp.where(keep, wide, 0.0).astype(BF16)


def flipped(me, k):
    out = 0
    for bit in (1, 2, 4):
        b = (me // bit) % 2
        out = out + bit * (1 - b if k & bit else b)
    return out


def exchange_kernel(n, n_dev, rows, a_hbm, c_ref, *refs):
    n_got, n_tile = n_dev - len(DIAGONAL), len(TILES)
    got, tiles = refs[:n_got], refs[n_got:n_got + len(DIAGONAL) * n_tile]
    (a_buf, t1_ref, g_ref, l1_ref, r2_ref, ct_ref, a_sem, chunk_sem, own_sem, tile_sem, send_sem,
     recv_sem) = refs[n_got + len(tiles):]
    nj = n // n_dev
    me = lax.axis_index('dev')
    barrier = pltpu.get_barrier_semaphore()
    for k in DIRECT:
        pl.semaphore_signal(barrier, inc=1, device_id={'dev': flipped(me, k)}, device_id_type=pl.DeviceIdType.MESH)

    def chunk(g):
        q = pl.ds(g * 16, 16)
        return pltpu.make_async_copy(a_hbm.at[0, q], a_buf.at[0, q], chunk_sem.at[g])

    def fetch(i):
        slot = lax.rem(i, 2)
        return pltpu.make_async_copy(a_hbm.at[i], a_buf.at[slot], a_sem.at[slot])

    for g in range(n // 16):
        chunk(g).start()
    build_small(n, c_ref, r2_ref, ct_ref)
    for k in DIRECT[:2]:
        build_l1(n, flipped(me, k) * nj, nj, ct_ref, l1_ref)
    zero = jnp.zeros((8 * n, 128 - n), BF16)

    def remote(k, src, dst):
        return pltpu.make_async_remote_copy(
            src_ref=src, dst_ref=dst, send_sem=send_sem.at[k], recv_sem=recv_sem.at[k],
            device_id={'dev': flipped(me, k)}, device_id_type=pl.DeviceIdType.MESH)

    def tile_copies(k, rows_):
        x = DIAGONAL.index(k)
        for t, (a0, size, lane, lanes) in enumerate(TILES):
            j = x * n_tile + t
            src = g_ref.at[k, rows_, pl.ds(a0, size), pl.ds(lane, lanes)]
            yield pltpu.make_async_copy(src, tiles[j].at[rows_], tile_sem.at[j])

    def send(k, i):
        if k == 0:
            pltpu.make_async_copy(g_ref.at[0, i], got[0].at[i], own_sem).start()
        elif k in DIAGONAL:
            for copy in tile_copies(k, i):
                copy.start()
        else:
            remote(k, g_ref.at[k, i], got[k].at[i]).start()

    def step_one(slot, g, lhs):
        q0 = pl.multiple_of(g * 16, 16)
        lo = a_buf[slot, pl.ds(q0, 8)].reshape(8 * n, n)
        hi = a_buf[slot, pl.ds(q0 + 8, 8)].reshape(8 * n, n)
        t = dot(lhs, jnp.concatenate([lo, zero, hi, zero], axis=1))
        nj = t.shape[0] // 8
        t = jnp.concatenate([t[:, :128].reshape(nj, 8, 128), t[:, 128:].reshape(nj, 8, 128)], axis=1)
        return pl.ds(q0, 16), t.astype(BF16)

    def step_two_three(k, i):
        d = flipped(me, k)
        t = t1_ref[pl.ds(d * nj, nj)].reshape(nj // 4, 4, n, 128)
        lhs = jnp.concatenate([t[:, jj].reshape(nj // 4 * n, 128) for jj in range(4)], axis=1)
        h = dot(lhs, r2_ref[...]).astype(BF16)
        h = jnp.concatenate([h[g * n:(g + 1) * n] for g in range(nj // 4)], axis=1)
        g_ref[k, i] = dot(ct_ref[...], h).astype(BF16)

    def some(ks, i, slot, wait):
        def first(g, carry):
            if wait:
                chunk(g).wait()
            lhs = jnp.concatenate(
                [l1_ref[pl.ds(pl.multiple_of(flipped(me, k) * 8 * nj, 8 * nj), 8 * nj)] for k in ks], axis=0)
            q, t = step_one(slot, g, lhs)
            for x, k in enumerate(ks):
                t1_ref[pl.ds(flipped(me, k) * nj, nj), q, :] = t[x * nj:(x + 1) * nj]
            return carry

        lax.fori_loop(0, n // 16, first, 0)
        before = None
        for k in ks:
            step_two_three(k, i)
            if before is not None:
                send(before, i)
            elif wait:
                pl.semaphore_wait(barrier, len(DIRECT))
            before = k
        send(before, i)

    some(DIRECT[:2], 0, 0, True)
    fetch(1).start()
    build_l1(n, 0, n, ct_ref, l1_ref)
    some((*DIRECT[2:], 0, *DIAGONAL), 0, 0, False)

    def row(i, carry):
        slot = lax.rem(i, 2)
        fetch(i).wait()

        @pl.when(i + 1 < rows)
        def _():
            fetch(i + 1).start()

        def first(g, carry):
            q, t = step_one(slot, g, l1_ref[...])
            t1_ref[:, q, :] = t
            return carry

        lax.fori_loop(0, n // 16, first, 0)
        before = None
        for k in (*DIRECT, 0, *DIAGONAL):
            step_two_three(k, i)
            if before is not None:
                send(before, i)
            before = k
        send(before, i)
        return carry

    lax.fori_loop(1, rows, row, 0)
    pltpu.make_async_copy(g_ref.at[0], got[0], own_sem).wait()
    for k in DIAGONAL:
        for copy in tile_copies(k, pl.ds(0, rows)):
            copy.wait()
    for k in DIRECT:
        remote(k, g_ref.at[k], got[k]).wait()


def out_kernel(n_in, wide, *refs):
    l4_ref, out_ref = refs[n_in], refs[-1]
    rhs = jnp.concatenate([r[...].reshape(-1, wide) for r in refs[:n_in]], axis=0)
    out_ref[...] = dot(l4_ref[...], rhs).reshape(out_ref.shape)


def tail_kernel(n, rows, at, a0, lane, lanes, parts, *refs):
    blocks, l4_hbm = refs[:len(at)], refs[len(at)]
    out_hbm, rhs_ref, l4_ref, v_ref, in_sem, l4_sem, out_sem = refs[-7:]
    size = n // parts
    loads = []
    for x, (block, (a, first)) in enumerate(zip(blocks, at)):
        loads.append(pltpu.make_async_copy(
            block.at[:, pl.ds(a, 8), pl.ds(first, lanes)], rhs_ref.at[pl.ds(x * rows, rows)], in_sem.at[x]))
    l4_loads = []
    for x in range(parts):
        i = pl.ds(8 * size * x, 8 * size)
        l4_loads.append(pltpu.make_async_copy(l4_hbm.at[i], l4_ref.at[i], l4_sem.at[x]))
    for copy in (*loads, *l4_loads):
        copy.start()
    for copy in loads:
        copy.wait()
    rhs = rhs_ref[...].reshape(8 * n, lanes)
    copies = []
    for x in range(parts):
        i = pl.ds(x * size, size)
        l4_loads[x].wait()
        v_ref[i] = dot(l4_ref[pl.ds(8 * size * x, 8 * size)], rhs).reshape(size, 8, lanes)
        copies.append(pltpu.make_async_copy(
            v_ref.at[i], out_hbm.at[i, pl.ds(a0, 8), pl.ds(lane, lanes)], out_sem.at[x]))
        copies[-1].start()
    for copy in copies:
        copy.wait()


def solution(mesh):
    n_dev = mesh.shape['dev']

    def transform(ao_rows, coeffs):
        rows = ao_rows.shape[0]
        n = coeffs.shape[0]
        wide = n * n // n_dev
        me_arr = jnp.full((1,), lax.axis_index('dev'), jnp.int32)
        smem = pl.BlockSpec(memory_space=pltpu.SMEM)
        vmem = pl.BlockSpec(memory_space=pltpu.VMEM)
        hbm = pl.BlockSpec(memory_space=pl.ANY)

        def const(shape):
            return pl.BlockSpec(shape, lambda *_: (0,) * len(shape))

        square, second = (8 * n, 8 * n), (512, 4 * n)
        n_got = n_dev - len(DIAGONAL)
        shapes = [(rows, n, wide)] * n_got
        shapes += [(rows, size, lanes) for _ in DIAGONAL for _, size, _, lanes in TILES]
        outs = pl.pallas_call(
            functools.partial(exchange_kernel, n, n_dev, rows),
            in_specs=[hbm, vmem],
            out_specs=[hbm] * len(shapes),
            out_shape=[jax.ShapeDtypeStruct(s, BF16) for s in shapes],
            scratch_shapes=[
                pltpu.VMEM((2, n, n, n), BF16), pltpu.VMEM((n, n, 128), BF16),
                pltpu.VMEM((n_dev, rows, n, wide), BF16), pltpu.VMEM(square, BF16),
                pltpu.VMEM(second, BF16), pltpu.VMEM((n, n), BF16),
                pltpu.SemaphoreType.DMA((2,)), pltpu.SemaphoreType.DMA((n // 16,)), pltpu.SemaphoreType.DMA,
                pltpu.SemaphoreType.DMA((len(shapes) - n_got,)),
                pltpu.SemaphoreType.DMA((n_dev,)), pltpu.SemaphoreType.DMA((n_dev,))],
            compiler_params=pltpu.CompilerParams(collective_id=0, has_side_effects=True),
            name='exchange',
        )(ao_rows, coeffs)
        got, tiles = outs[:n_got], outs[n_got:]
        moved = {}
        for t in range(len(TILES)):
            for x, k in enumerate(DIAGONAL):
                moved[k, t] = lax.ppermute(
                    tiles[x * len(TILES) + t], 'dev', [(i, i ^ k) for i in range(n_dev)])
        l4 = pl.pallas_call(
            functools.partial(last_kernel, n, rows),
            in_specs=[smem, vmem, hbm],
            out_specs=vmem,
            out_shape=jax.ShapeDtypeStruct(square, BF16),
            name='last',
        )(me_arr, coeffs, got[0])

        out = None
        for t_i, (a0, size, lane, lanes) in enumerate(TILES):
            ins, specs, ats = [], [], []
            for k in range(n_dev):
                block, at = (moved[k, t_i], (0, 0)) if (k, t_i) in moved else (got[k], (a0, lane))
                ins.append(block)
                ats.append(at)
                specs.append(pl.BlockSpec((pl.Element(rows), pl.Element(8), pl.Element(lanes)), lambda i, at=at: (0, pl.multiple_of(at[0] + 8 * i, 8), at[1])))
            n_in = len(ins)
            ins.append(l4)
            specs.append(const(square))
            if out is not None:
                ins.append(out)
                specs.append(hbm)
            alone, parts = size == 8, 3
            if alone:
                specs = [hbm] * len(specs)
            out = pl.pallas_call(
                functools.partial(tail_kernel, n, rows, ats, a0, lane, lanes, parts) if alone
                else functools.partial(out_kernel, n_in, lanes),
                grid=(size // 8,),
                in_specs=specs,
                out_specs=hbm if alone else pl.BlockSpec(
                    (pl.Element(n), pl.Element(8), pl.Element(lanes)),
                    lambda i, at=(a0, lane): (0, pl.multiple_of(at[0] + 8 * i, 8), at[1])),
                out_shape=jax.ShapeDtypeStruct((n, n, wide), F32),
                input_output_aliases={} if t_i == 0 else {len(ins) - 1: 0},
                scratch_shapes=[
                    pltpu.VMEM((n, 8, lanes), BF16), pltpu.VMEM(square, BF16), pltpu.VMEM((n, 8, lanes), F32),
                    pltpu.SemaphoreType.DMA((n_dev,)), pltpu.SemaphoreType.DMA((parts,)),
                    pltpu.SemaphoreType.DMA((parts,))] * alone,
                compiler_params=pltpu.CompilerParams(vmem_limit_bytes=67043328),
                name='out',
            )(*ins)
        return out

    return jax.shard_map(transform, mesh=mesh, in_specs=(P(('frag', 'dev')), P('frag')), out_specs=P('frag', None, 'dev'), check_vma=False)
```

```python
import functools

import jax
import jax.numpy as jnp
from jax import lax
from jax.experimental import pallas as pl
from jax.experimental.pallas import tpu as pltpu
from jax.sharding import PartitionSpec as P


TILES = ((0, 48, 0, 1152), (48, 24, 0, 1152), (72, 8, 0, 1152), (80, 8, 0, 1152), (88, 8, 0, 640), (88, 8, 640, 512))
DIAGONAL = (6, 7)
DIRECT = (2, 4, 3, 5, 1)
F32, BF16 = jnp.float32, jnp.bfloat16


def one_hot(shape, fn):
    rows = lax.broadcasted_iota(jnp.int32, shape, 0)
    cols = lax.broadcasted_iota(jnp.int32, shape, 1)
    return fn(rows, cols)


def dot(a, b):
    return jnp.dot(a, b, preferred_element_type=F32)


def pick(shape, fn):
    return one_hot(shape, fn).astype(BF16)


def transposed(c, n):
    eye = pick((n, n), lambda i, j: i == j)
    return lax.dot_general(c, eye, (((0,), (0,)), ((), ())), preferred_element_type=F32).astype(BF16)


def build_first(n, c_ref, l1_ref, r2_ref, ct_ref):
    c = c_ref[...]
    ct = transposed(c, n)
    ct_ref[...] = ct
    tall = dot(pick((8 * n, n), lambda i, j: i // 8 == j), ct).astype(BF16)
    wide = dot(tall, pick((n, 8 * n), lambda i, j: j % n == i))
    keep = one_hot((8 * n, 8 * n), lambda i, j: i % 8 == j // n)
    l1_ref[...] = jnp.where(keep, wide, 0.0).astype(BF16)
    tall = dot(pick((512, n), lambda i, j: i % 128 == j), c).astype(BF16)
    wide = dot(tall, pick((n, 4 * n), lambda i, j: j % n == i))
    keep = one_hot((512, 4 * n), lambda i, j: i // 128 == j // n)
    r2_ref[...] = jnp.where(keep, wide, 0.0).astype(BF16)


def last_kernel(n, rows, me_ref, c_ref, after_ref, l4_ref):
    me = me_ref[0]

    def source(r, col):
        m = col // 8
        return r == (me ^ (m // rows)) * rows + m % rows

    ct = transposed(c_ref[...], n)
    tall = dot(pick((8 * n, n), lambda i, j: i // 8 == j), ct).astype(BF16)
    wide = dot(tall, pick((n, 8 * n), source))
    keep = one_hot((8 * n, 8 * n), lambda i, j: i % 8 == j % 8)
    l4_ref[...] = jnp.where(keep, wide, 0.0).astype(BF16)


def flipped(me, k):
    out = 0
    for bit in (1, 2, 4):
        b = (me // bit) % 2
        out = out + bit * (1 - b if k & bit else b)
    return out


def exchange_kernel(n, n_dev, rows, a_hbm, c_hbm, *refs):
    n_got, n_tile = n_dev - len(DIAGONAL), len(TILES)
    got, tiles = refs[:n_got], refs[n_got:n_got + len(DIAGONAL) * n_tile]
    (a_buf, c_ref, t1_ref, g_ref, l1_ref, r2_ref, ct_ref, c_sem, a_sem, chunk_sem, own_sem, tile_sem, send_sem,
     recv_sem) = refs[n_got + len(tiles):]
    nj = n // n_dev
    me = lax.axis_index('dev')

    def chunk(g):
        q = pl.ds(g * 16, 16)
        return pltpu.make_async_copy(a_hbm.at[0, q], a_buf.at[0, q], chunk_sem.at[g])

    def fetch(i):
        slot = lax.rem(i, 2)
        return pltpu.make_async_copy(a_hbm.at[i], a_buf.at[slot], a_sem.at[slot])

    c_copy = pltpu.make_async_copy(c_hbm, c_ref, c_sem)
    c_copy.start()
    for g in range(n // 16):
        chunk(g).start()
    fetch(1).start()
    barrier = pltpu.get_barrier_semaphore()
    for k in DIRECT:
        pl.semaphore_signal(barrier, inc=1, device_id={'dev': flipped(me, k)}, device_id_type=pl.DeviceIdType.MESH)
    c_copy.wait()
    build_first(n, c_ref, l1_ref, r2_ref, ct_ref)
    zero = jnp.zeros((8 * n, 128 - n), BF16)

    def remote(k, src, dst):
        return pltpu.make_async_remote_copy(
            src_ref=src, dst_ref=dst, send_sem=send_sem.at[k], recv_sem=recv_sem.at[k],
            device_id={'dev': flipped(me, k)}, device_id_type=pl.DeviceIdType.MESH)

    def tile_copies(k, rows_):
        x = DIAGONAL.index(k)
        for t, (a0, size, lane, lanes) in enumerate(TILES):
            j = x * n_tile + t
            src = g_ref.at[k, rows_, pl.ds(a0, size), pl.ds(lane, lanes)]
            yield pltpu.make_async_copy(src, tiles[j].at[rows_], tile_sem.at[j])

    def send(k, i):
        if k == 0:
            pltpu.make_async_copy(g_ref.at[0, i], got[0].at[i], own_sem).start()
        elif k in DIAGONAL:
            for copy in tile_copies(k, i):
                copy.start()
        else:
            remote(k, g_ref.at[k, i], got[k].at[i]).start()

    def step_one(slot, g, lhs):
        q0 = pl.multiple_of(g * 16, 16)
        lo = a_buf[slot, pl.ds(q0, 8)].reshape(8 * n, n)
        hi = a_buf[slot, pl.ds(q0 + 8, 8)].reshape(8 * n, n)
        t = dot(lhs, jnp.concatenate([lo, zero, hi, zero], axis=1))
        nj = t.shape[0] // 8
        t = jnp.concatenate([t[:, :128].reshape(nj, 8, 128), t[:, 128:].reshape(nj, 8, 128)], axis=1)
        return pl.ds(q0, 16), t.astype(BF16)

    def step_two_three(k, i):
        d = flipped(me, k)
        t = t1_ref[pl.ds(d * nj, nj)].reshape(nj // 4, 4, n, 128)
        lhs = jnp.concatenate([t[:, jj].reshape(nj // 4 * n, 128) for jj in range(4)], axis=1)
        h = dot(lhs, r2_ref[...]).astype(BF16)
        h = jnp.concatenate([h[g * n:(g + 1) * n] for g in range(nj // 4)], axis=1)
        g_ref[k, i] = dot(ct_ref[...], h).astype(BF16)

    def some(ks, i, slot, wait):
        def first(pair, carry):
            if wait:
                chunk(2 * pair).wait()
                chunk(2 * pair + 1).wait()
            lhs = jnp.concatenate(
                [l1_ref[pl.ds(pl.multiple_of(flipped(me, k) * 8 * nj, 8 * nj), 8 * nj)] for k in ks], axis=0)
            for g in range(2):
                q, t = step_one(slot, 2 * pair + g, lhs)
                for x, k in enumerate(ks):
                    t1_ref[pl.ds(flipped(me, k) * nj, nj), q, :] = t[x * nj:(x + 1) * nj]
            return carry

        lax.fori_loop(0, n // 32, first, 0)
        for k in ks:
            step_two_three(k, i)
        if wait:
            pl.semaphore_wait(barrier, len(DIRECT))
        for k in ks:
            send(k, i)

    some(DIRECT[:2], 0, 0, True)
    some((*DIRECT[2:], 0, *DIAGONAL), 0, 0, False)

    def row(i, carry):
        slot = lax.rem(i, 2)
        fetch(i).wait()

        @pl.when(i + 1 < rows)
        def _():
            fetch(i + 1).start()

        def first(g, carry):
            q, t = step_one(slot, g, l1_ref[...])
            t1_ref[:, q, :] = t
            return carry

        lax.fori_loop(0, n // 16, first, 0)
        before = None
        for k in (*DIRECT, 0, *DIAGONAL):
            step_two_three(k, i)
            if before is not None:
                send(before, i)
            before = k
        send(before, i)
        return carry

    lax.fori_loop(1, rows, row, 0)
    pltpu.make_async_copy(g_ref.at[0], got[0], own_sem).wait()
    for k in DIAGONAL:
        for copy in tile_copies(k, pl.ds(0, rows)):
            copy.wait()
    for k in DIRECT:
        remote(k, g_ref.at[k], got[k]).wait()


def out_kernel(n_in, wide, *refs):
    l4_ref, out_ref = refs[n_in], refs[-1]
    rhs = jnp.concatenate([r[...].reshape(-1, wide) for r in refs[:n_in]], axis=0)
    out_ref[...] = dot(l4_ref[...], rhs).reshape(out_ref.shape)


def tail_kernel(n, n_in, a0, lane, lanes, parts, *refs):
    l4_ref, out_hbm, (v_ref, sem) = refs[n_in], refs[-3], refs[-2:]
    rhs = jnp.concatenate([r[...].reshape(-1, lanes) for r in refs[:n_in]], axis=0)
    size = n // parts
    copies = []
    for x in range(parts):
        i = pl.ds(x * size, size)
        v_ref[i] = dot(l4_ref[pl.ds(8 * size * x, 8 * size)], rhs).reshape(size, 8, lanes)
        copies.append(pltpu.make_async_copy(
            v_ref.at[i], out_hbm.at[i, pl.ds(a0, 8), pl.ds(lane, lanes)], sem.at[x]))
        copies[-1].start()
    for copy in copies:
        copy.wait()


def solution(mesh):
    n_dev = mesh.shape['dev']

    def transform(ao_rows, coeffs):
        rows = ao_rows.shape[0]
        n = coeffs.shape[0]
        wide = n * n // n_dev
        me_arr = jnp.full((1,), lax.axis_index('dev'), jnp.int32)
        smem = pl.BlockSpec(memory_space=pltpu.SMEM)
        vmem = pl.BlockSpec(memory_space=pltpu.VMEM)
        hbm = pl.BlockSpec(memory_space=pl.ANY)

        def const(shape):
            return pl.BlockSpec(shape, lambda *_: (0,) * len(shape))

        square, second = (8 * n, 8 * n), (512, 4 * n)
        n_got = n_dev - len(DIAGONAL)
        shapes = [(rows, n, wide)] * n_got
        shapes += [(rows, size, lanes) for _ in DIAGONAL for _, size, _, lanes in TILES]
        outs = pl.pallas_call(
            functools.partial(exchange_kernel, n, n_dev, rows),
            in_specs=[hbm, hbm],
            out_specs=[hbm] * len(shapes),
            out_shape=[jax.ShapeDtypeStruct(s, BF16) for s in shapes],
            scratch_shapes=[
                pltpu.VMEM((2, n, n, n), BF16), pltpu.VMEM((n, n), BF16), pltpu.VMEM((n, n, 128), BF16),
                pltpu.VMEM((n_dev, rows, n, wide), BF16), pltpu.VMEM(square, BF16),
                pltpu.VMEM(second, BF16), pltpu.VMEM((n, n), BF16),
                pltpu.SemaphoreType.DMA, pltpu.SemaphoreType.DMA((2,)), pltpu.SemaphoreType.DMA((n // 16,)), pltpu.SemaphoreType.DMA,
                pltpu.SemaphoreType.DMA((len(shapes) - n_got,)),
                pltpu.SemaphoreType.DMA((n_dev,)), pltpu.SemaphoreType.DMA((n_dev,))],
            compiler_params=pltpu.CompilerParams(collective_id=0, has_side_effects=True),
            name='exchange',
        )(ao_rows, coeffs)
        got, tiles = outs[:n_got], outs[n_got:]
        moved = {}
        for t in range(len(TILES)):
            for x, k in enumerate(DIAGONAL):
                moved[k, t] = lax.ppermute(
                    tiles[x * len(TILES) + t], 'dev', [(i, i ^ k) for i in range(n_dev)])
        l4 = pl.pallas_call(
            functools.partial(last_kernel, n, rows),
            in_specs=[smem, vmem, hbm],
            out_specs=vmem,
            out_shape=jax.ShapeDtypeStruct(square, BF16),
            name='last',
        )(me_arr, coeffs, got[0])

        out = None
        for t_i, (a0, size, lane, lanes) in enumerate(TILES):
            ins, specs = [], []
            for k in range(n_dev):
                block, at = (moved[k, t_i], (0, 0)) if (k, t_i) in moved else (got[k], (a0, lane))
                ins.append(block)
                specs.append(pl.BlockSpec((pl.Element(rows), pl.Element(8), pl.Element(lanes)), lambda i, at=at: (0, pl.multiple_of(at[0] + 8 * i, 8), at[1])))
            n_in = len(ins)
            ins.append(l4)
            specs.append(const(square))
            if out is not None:
                ins.append(out)
                specs.append(hbm)
            alone = size == 8
            out = pl.pallas_call(
                functools.partial(tail_kernel, n, n_in, a0, lane, lanes, 4) if alone
                else functools.partial(out_kernel, n_in, lanes),
                grid=(size // 8,),
                in_specs=specs,
                out_specs=hbm if alone else pl.BlockSpec(
                    (pl.Element(n), pl.Element(8), pl.Element(lanes)),
                    lambda i, at=(a0, lane): (0, pl.multiple_of(at[0] + 8 * i, 8), at[1])),
                out_shape=jax.ShapeDtypeStruct((n, n, wide), F32),
                input_output_aliases={} if t_i == 0 else {len(ins) - 1: 0},
                scratch_shapes=[pltpu.VMEM((n, 8, lanes), F32), pltpu.SemaphoreType.DMA((4,))] * alone,
                compiler_params=pltpu.CompilerParams(vmem_limit_bytes=67043328),
                name='out',
            )(*ins)
        return out

    return jax.shard_map(transform, mesh=mesh, in_specs=(P(('frag', 'dev')), P('frag')), out_specs=P('frag', None, 'dev'), check_vma=False)
```

```python
import functools

import jax
import jax.numpy as jnp
from jax import lax
from jax.experimental import pallas as pl
from jax.experimental.pallas import tpu as pltpu
from jax.sharding import PartitionSpec as P


TILES = ((0, 48, 0, 1152), (48, 24, 0, 1152), (72, 8, 0, 1152), (80, 8, 0, 1152), (88, 8, 0, 640), (88, 8, 640, 512))
DIAGONAL = (6, 7)
DIRECT = (2, 4, 3, 5, 1)
F32, BF16 = jnp.float32, jnp.bfloat16


def one_hot(shape, fn):
    rows = lax.broadcasted_iota(jnp.int32, shape, 0)
    cols = lax.broadcasted_iota(jnp.int32, shape, 1)
    return fn(rows, cols)


def dot(a, b):
    return jnp.dot(a, b, preferred_element_type=F32)


def pick(shape, fn):
    return one_hot(shape, fn).astype(BF16)


def transposed(c, n):
    eye = pick((n, n), lambda i, j: i == j)
    return lax.dot_general(c, eye, (((0,), (0,)), ((), ())), preferred_element_type=F32).astype(BF16)


def build_first(n, c_ref, l1_ref, r2_ref, ct_ref):
    c = c_ref[...]
    ct = transposed(c, n)
    ct_ref[...] = ct
    tall = dot(pick((8 * n, n), lambda i, j: i // 8 == j), ct).astype(BF16)
    wide = dot(tall, pick((n, 8 * n), lambda i, j: j % n == i))
    keep = one_hot((8 * n, 8 * n), lambda i, j: i % 8 == j // n)
    l1_ref[...] = jnp.where(keep, wide, 0.0).astype(BF16)
    tall = dot(pick((512, n), lambda i, j: i % 128 == j), c).astype(BF16)
    wide = dot(tall, pick((n, 4 * n), lambda i, j: j % n == i))
    keep = one_hot((512, 4 * n), lambda i, j: i // 128 == j // n)
    r2_ref[...] = jnp.where(keep, wide, 0.0).astype(BF16)


def last_kernel(n, rows, me_ref, c_ref, after_ref, l4_ref):
    me = me_ref[0]

    def source(r, col):
        m = col // 8
        return r == (me ^ (m // rows)) * rows + m % rows

    ct = transposed(c_ref[...], n)
    tall = dot(pick((8 * n, n), lambda i, j: i // 8 == j), ct).astype(BF16)
    wide = dot(tall, pick((n, 8 * n), source))
    keep = one_hot((8 * n, 8 * n), lambda i, j: i % 8 == j % 8)
    l4_ref[...] = jnp.where(keep, wide, 0.0).astype(BF16)


def flipped(me, k):
    out = 0
    for bit in (1, 2, 4):
        b = (me // bit) % 2
        out = out + bit * (1 - b if k & bit else b)
    return out


def exchange_kernel(n, n_dev, rows, a_hbm, c_ref, *refs):
    n_got, n_tile = n_dev - len(DIAGONAL), len(TILES)
    got, tiles = refs[:n_got], refs[n_got:n_got + len(DIAGONAL) * n_tile]
    (a_buf, t1_ref, g_ref, l1_ref, r2_ref, ct_ref, a_sem, chunk_sem, own_sem, tile_sem, send_sem,
     recv_sem) = refs[n_got + len(tiles):]
    nj = n // n_dev
    me = lax.axis_index('dev')
    barrier = pltpu.get_barrier_semaphore()
    for k in DIRECT:
        pl.semaphore_signal(barrier, inc=1, device_id={'dev': flipped(me, k)}, device_id_type=pl.DeviceIdType.MESH)

    def chunk(g):
        q = pl.ds(g * 16, 16)
        return pltpu.make_async_copy(a_hbm.at[0, q], a_buf.at[0, q], chunk_sem.at[g])

    def fetch(i):
        slot = lax.rem(i, 2)
        return pltpu.make_async_copy(a_hbm.at[i], a_buf.at[slot], a_sem.at[slot])

    for g in range(n // 16):
        chunk(g).start()
    fetch(1).start()
    build_first(n, c_ref, l1_ref, r2_ref, ct_ref)
    zero = jnp.zeros((8 * n, 128 - n), BF16)

    def remote(k, src, dst):
        return pltpu.make_async_remote_copy(
            src_ref=src, dst_ref=dst, send_sem=send_sem.at[k], recv_sem=recv_sem.at[k],
            device_id={'dev': flipped(me, k)}, device_id_type=pl.DeviceIdType.MESH)

    def tile_copies(k, rows_):
        x = DIAGONAL.index(k)
        for t, (a0, size, lane, lanes) in enumerate(TILES):
            j = x * n_tile + t
            src = g_ref.at[k, rows_, pl.ds(a0, size), pl.ds(lane, lanes)]
            yield pltpu.make_async_copy(src, tiles[j].at[rows_], tile_sem.at[j])

    def send(k, i):
        if k == 0:
            pltpu.make_async_copy(g_ref.at[0, i], got[0].at[i], own_sem).start()
        elif k in DIAGONAL:
            for copy in tile_copies(k, i):
                copy.start()
        else:
            remote(k, g_ref.at[k, i], got[k].at[i]).start()

    def step_one(slot, g, lhs):
        q0 = pl.multiple_of(g * 16, 16)
        lo = a_buf[slot, pl.ds(q0, 8)].reshape(8 * n, n)
        hi = a_buf[slot, pl.ds(q0 + 8, 8)].reshape(8 * n, n)
        t = dot(lhs, jnp.concatenate([lo, zero, hi, zero], axis=1))
        nj = t.shape[0] // 8
        t = jnp.concatenate([t[:, :128].reshape(nj, 8, 128), t[:, 128:].reshape(nj, 8, 128)], axis=1)
        return pl.ds(q0, 16), t.astype(BF16)

    def step_two_three(k, i, d=None):
        d = flipped(me, k) if d is None else d
        t = t1_ref[pl.ds(d * nj, nj)].reshape(nj // 4, 4, n, 128)
        lhs = jnp.concatenate([t[:, jj].reshape(nj // 4 * n, 128) for jj in range(4)], axis=1)
        h = dot(lhs, r2_ref[...]).astype(BF16)
        h = jnp.concatenate([h[g * n:(g + 1) * n] for g in range(nj // 4)], axis=1)
        g_ref[k, i] = dot(ct_ref[...], h).astype(BF16)

    def some(ks, i, slot, wait):
        def first(pair, carry):
            if wait:
                chunk(2 * pair).wait()
                chunk(2 * pair + 1).wait()
            lhs = jnp.concatenate(
                [l1_ref[pl.ds(pl.multiple_of(flipped(me, k) * 8 * nj, 8 * nj), 8 * nj)] for k in ks], axis=0)
            for g in range(2):
                q, t = step_one(slot, 2 * pair + g, lhs)
                for x, k in enumerate(ks):
                    t1_ref[pl.ds(flipped(me, k) * nj, nj), q, :] = t[x * nj:(x + 1) * nj]
            return carry

        lax.fori_loop(0, n // 32, first, 0)
        if not wait:
            for k in ks:
                step_two_three(k, i)
            for k in ks:
                send(k, i)
            return
        core = me % 2
        (k0, d0), (k1, d1) = ((k, flipped(me, k)) for k in ks)
        for turn in range(2):
            swap = core if turn == 0 else 1 - core
            step_two_three(k0 + swap * (k1 - k0), i, d0 + swap * (d1 - d0))
            if turn == 0:
                pl.semaphore_wait(barrier, len(DIRECT))
            for x, k in enumerate(ks):
                @pl.when(swap == x)
                def _(k=k):
                    send(k, i)

    some(DIRECT[:2], 0, 0, True)
    some((*DIRECT[2:], 0, *DIAGONAL), 0, 0, False)

    def row(i, carry):
        slot = lax.rem(i, 2)
        fetch(i).wait()

        @pl.when(i + 1 < rows)
        def _():
            fetch(i + 1).start()

        def first(g, carry):
            q, t = step_one(slot, g, l1_ref[...])
            t1_ref[:, q, :] = t
            return carry

        lax.fori_loop(0, n // 16, first, 0)
        before = None
        for k in (*DIRECT, 0, *DIAGONAL):
            step_two_three(k, i)
            if before is not None:
                send(before, i)
            before = k
        send(before, i)
        return carry

    lax.fori_loop(1, rows, row, 0)
    pltpu.make_async_copy(g_ref.at[0], got[0], own_sem).wait()
    for k in DIAGONAL:
        for copy in tile_copies(k, pl.ds(0, rows)):
            copy.wait()
    for k in DIRECT:
        remote(k, g_ref.at[k], got[k]).wait()


def out_kernel(n_in, wide, *refs):
    l4_ref, out_ref = refs[n_in], refs[-1]
    rhs = jnp.concatenate([r[...].reshape(-1, wide) for r in refs[:n_in]], axis=0)
    out_ref[...] = dot(l4_ref[...], rhs).reshape(out_ref.shape)


def tail_kernel(n, n_in, a0, lane, lanes, parts, *refs):
    l4_ref, out_hbm, (v_ref, sem) = refs[n_in], refs[-3], refs[-2:]
    rhs = jnp.concatenate([r[...].reshape(-1, lanes) for r in refs[:n_in]], axis=0)
    size = n // parts
    copies = []
    for x in range(parts):
        i = pl.ds(x * size, size)
        v_ref[i] = dot(l4_ref[pl.ds(8 * size * x, 8 * size)], rhs).reshape(size, 8, lanes)
        copies.append(pltpu.make_async_copy(
            v_ref.at[i], out_hbm.at[i, pl.ds(a0, 8), pl.ds(lane, lanes)], sem.at[x]))
        copies[-1].start()
    for copy in copies:
        copy.wait()


def solution(mesh):
    n_dev = mesh.shape['dev']

    def transform(ao_rows, coeffs):
        rows = ao_rows.shape[0]
        n = coeffs.shape[0]
        wide = n * n // n_dev
        me_arr = jnp.full((1,), lax.axis_index('dev'), jnp.int32)
        smem = pl.BlockSpec(memory_space=pltpu.SMEM)
        vmem = pl.BlockSpec(memory_space=pltpu.VMEM)
        hbm = pl.BlockSpec(memory_space=pl.ANY)

        def const(shape):
            return pl.BlockSpec(shape, lambda *_: (0,) * len(shape))

        square, second = (8 * n, 8 * n), (512, 4 * n)
        n_got = n_dev - len(DIAGONAL)
        shapes = [(rows, n, wide)] * n_got
        shapes += [(rows, size, lanes) for _ in DIAGONAL for _, size, _, lanes in TILES]
        outs = pl.pallas_call(
            functools.partial(exchange_kernel, n, n_dev, rows),
            in_specs=[hbm, vmem],
            out_specs=[hbm] * len(shapes),
            out_shape=[jax.ShapeDtypeStruct(s, BF16) for s in shapes],
            scratch_shapes=[
                pltpu.VMEM((2, n, n, n), BF16), pltpu.VMEM((n, n, 128), BF16),
                pltpu.VMEM((n_dev, rows, n, wide), BF16), pltpu.VMEM(square, BF16),
                pltpu.VMEM(second, BF16), pltpu.VMEM((n, n), BF16),
                pltpu.SemaphoreType.DMA((2,)), pltpu.SemaphoreType.DMA((n // 16,)), pltpu.SemaphoreType.DMA,
                pltpu.SemaphoreType.DMA((len(shapes) - n_got,)),
                pltpu.SemaphoreType.DMA((n_dev,)), pltpu.SemaphoreType.DMA((n_dev,))],
            compiler_params=pltpu.CompilerParams(collective_id=0, has_side_effects=True),
            name='exchange',
        )(ao_rows, coeffs)
        got, tiles = outs[:n_got], outs[n_got:]
        moved = {}
        for t in range(len(TILES)):
            for x, k in enumerate(DIAGONAL):
                moved[k, t] = lax.ppermute(
                    tiles[x * len(TILES) + t], 'dev', [(i, i ^ k) for i in range(n_dev)])
        l4 = pl.pallas_call(
            functools.partial(last_kernel, n, rows),
            in_specs=[smem, vmem, hbm],
            out_specs=vmem,
            out_shape=jax.ShapeDtypeStruct(square, BF16),
            name='last',
        )(me_arr, coeffs, got[0])

        out = None
        for t_i, (a0, size, lane, lanes) in enumerate(TILES):
            ins, specs = [], []
            for k in range(n_dev):
                block, at = (moved[k, t_i], (0, 0)) if (k, t_i) in moved else (got[k], (a0, lane))
                ins.append(block)
                specs.append(pl.BlockSpec((pl.Element(rows), pl.Element(8), pl.Element(lanes)), lambda i, at=at: (0, pl.multiple_of(at[0] + 8 * i, 8), at[1])))
            n_in = len(ins)
            ins.append(l4)
            specs.append(const(square))
            if out is not None:
                ins.append(out)
                specs.append(hbm)
            alone = size == 8
            out = pl.pallas_call(
                functools.partial(tail_kernel, n, n_in, a0, lane, lanes, 4) if alone
                else functools.partial(out_kernel, n_in, lanes),
                grid=(size // 8,),
                in_specs=specs,
                out_specs=hbm if alone else pl.BlockSpec(
                    (pl.Element(n), pl.Element(8), pl.Element(lanes)),
                    lambda i, at=(a0, lane): (0, pl.multiple_of(at[0] + 8 * i, 8), at[1])),
                out_shape=jax.ShapeDtypeStruct((n, n, wide), F32),
                input_output_aliases={} if t_i == 0 else {len(ins) - 1: 0},
                scratch_shapes=[pltpu.VMEM((n, 8, lanes), F32), pltpu.SemaphoreType.DMA((4,))] * alone,
                compiler_params=pltpu.CompilerParams(vmem_limit_bytes=67043328),
                name='out',
            )(*ins)
        return out

    return jax.shard_map(transform, mesh=mesh, in_specs=(P(('frag', 'dev')), P('frag')), out_specs=P('frag', None, 'dev'), check_vma=False)
```

```python
import functools

import jax
import jax.numpy as jnp
from jax import lax
from jax.experimental import pallas as pl
from jax.experimental.pallas import tpu as pltpu
from jax.sharding import PartitionSpec as P


TILES = ((0, 48, 0, 1152), (48, 24, 0, 1152), (72, 8, 0, 1152), (80, 8, 0, 1152), (88, 8, 0, 640), (88, 8, 640, 512))
DIAGONAL = (6, 7)
DIRECT = (2, 4, 3, 5, 1)
F32, BF16 = jnp.float32, jnp.bfloat16


def one_hot(shape, fn):
    rows = lax.broadcasted_iota(jnp.int32, shape, 0)
    cols = lax.broadcasted_iota(jnp.int32, shape, 1)
    return fn(rows, cols)


def dot(a, b):
    return jnp.dot(a, b, preferred_element_type=F32)


def pick(shape, fn):
    return one_hot(shape, fn).astype(BF16)


def transposed(c, n):
    eye = pick((n, n), lambda i, j: i == j)
    return lax.dot_general(c, eye, (((0,), (0,)), ((), ())), preferred_element_type=F32).astype(BF16)


def build_first(n, c_ref, l1_ref, r2_ref, ct_ref):
    c = c_ref[...]
    ct = transposed(c, n)
    ct_ref[...] = ct
    tall = dot(pick((8 * n, n), lambda i, j: i // 8 == j), ct).astype(BF16)
    wide = dot(tall, pick((n, 8 * n), lambda i, j: j % n == i))
    keep = one_hot((8 * n, 8 * n), lambda i, j: i % 8 == j // n)
    l1_ref[...] = jnp.where(keep, wide, 0.0).astype(BF16)
    tall = dot(pick((512, n), lambda i, j: i % 128 == j), c).astype(BF16)
    wide = dot(tall, pick((n, 4 * n), lambda i, j: j % n == i))
    keep = one_hot((512, 4 * n), lambda i, j: i // 128 == j // n)
    r2_ref[...] = jnp.where(keep, wide, 0.0).astype(BF16)


def last_kernel(n, rows, me_ref, c_ref, after_ref, l4_ref):
    me = me_ref[0]

    def source(r, col):
        m = col // 8
        return r == (me ^ (m // rows)) * rows + m % rows

    ct = transposed(c_ref[...], n)
    tall = dot(pick((8 * n, n), lambda i, j: i // 8 == j), ct).astype(BF16)
    wide = dot(tall, pick((n, 8 * n), source))
    keep = one_hot((8 * n, 8 * n), lambda i, j: i % 8 == j % 8)
    l4_ref[...] = jnp.where(keep, wide, 0.0).astype(BF16)


def flipped(me, k):
    out = 0
    for bit in (1, 2, 4):
        b = (me // bit) % 2
        out = out + bit * (1 - b if k & bit else b)
    return out


def exchange_kernel(n, n_dev, rows, a_hbm, c_ref, *refs):
    n_got, n_tile = n_dev - len(DIAGONAL), len(TILES)
    got, tiles = refs[:n_got], refs[n_got:n_got + len(DIAGONAL) * n_tile]
    (a_buf, t1_ref, g_ref, l1_ref, r2_ref, ct_ref, a_sem, chunk_sem, own_sem, tile_sem, send_sem,
     recv_sem) = refs[n_got + len(tiles):]
    nj = n // n_dev
    me = lax.axis_index('dev')
    barrier = pltpu.get_barrier_semaphore()
    for k in DIRECT:
        pl.semaphore_signal(barrier, inc=1, device_id={'dev': flipped(me, k)}, device_id_type=pl.DeviceIdType.MESH)

    def chunk(g):
        q = pl.ds(g * 16, 16)
        return pltpu.make_async_copy(a_hbm.at[0, q], a_buf.at[0, q], chunk_sem.at[g])

    def fetch(i):
        slot = lax.rem(i, 2)
        return pltpu.make_async_copy(a_hbm.at[i], a_buf.at[slot], a_sem.at[slot])

    for g in range(n // 16):
        chunk(g).start()
    fetch(1).start()
    build_first(n, c_ref, l1_ref, r2_ref, ct_ref)
    zero = jnp.zeros((8 * n, 128 - n), BF16)

    def remote(k, src, dst):
        return pltpu.make_async_remote_copy(
            src_ref=src, dst_ref=dst, send_sem=send_sem.at[k], recv_sem=recv_sem.at[k],
            device_id={'dev': flipped(me, k)}, device_id_type=pl.DeviceIdType.MESH)

    def tile_copies(k, rows_):
        x = DIAGONAL.index(k)
        for t, (a0, size, lane, lanes) in enumerate(TILES):
            j = x * n_tile + t
            src = g_ref.at[k, rows_, pl.ds(a0, size), pl.ds(lane, lanes)]
            yield pltpu.make_async_copy(src, tiles[j].at[rows_], tile_sem.at[j])

    def send(k, i):
        if k == 0:
            pltpu.make_async_copy(g_ref.at[0, i], got[0].at[i], own_sem).start()
        elif k in DIAGONAL:
            for copy in tile_copies(k, i):
                copy.start()
        else:
            remote(k, g_ref.at[k, i], got[k].at[i]).start()

    def step_one(slot, g, lhs):
        q0 = pl.multiple_of(g * 16, 16)
        lo = a_buf[slot, pl.ds(q0, 8)].reshape(8 * n, n)
        hi = a_buf[slot, pl.ds(q0 + 8, 8)].reshape(8 * n, n)
        t = dot(lhs, jnp.concatenate([lo, zero, hi, zero], axis=1))
        nj = t.shape[0] // 8
        t = jnp.concatenate([t[:, :128].reshape(nj, 8, 128), t[:, 128:].reshape(nj, 8, 128)], axis=1)
        return pl.ds(q0, 16), t.astype(BF16)

    def step_two_three(k, i, d=None):
        d = flipped(me, k) if d is None else d
        t = t1_ref[pl.ds(d * nj, nj)].reshape(nj // 4, 4, n, 128)
        lhs = jnp.concatenate([t[:, jj].reshape(nj // 4 * n, 128) for jj in range(4)], axis=1)
        h = dot(lhs, r2_ref[...]).astype(BF16)
        h = jnp.concatenate([h[g * n:(g + 1) * n] for g in range(nj // 4)], axis=1)
        g_ref[k, i] = dot(ct_ref[...], h).astype(BF16)

    def groups(i, *groups_):
        for ks in groups_:
            for k in ks:
                step_two_three(k, i)
            for k in ks:
                send(k, i)

    def some(ks, i, slot, wait):
        def first(pair, carry):
            if wait:
                chunk(2 * pair).wait()
                chunk(2 * pair + 1).wait()
            lhs = jnp.concatenate(
                [l1_ref[pl.ds(pl.multiple_of(flipped(me, k) * 8 * nj, 8 * nj), 8 * nj)] for k in ks], axis=0)
            for g in range(2):
                q, t = step_one(slot, 2 * pair + g, lhs)
                for x, k in enumerate(ks):
                    t1_ref[pl.ds(flipped(me, k) * nj, nj), q, :] = t[x * nj:(x + 1) * nj]
            return carry

        lax.fori_loop(0, n // 32, first, 0)
        if not wait:
            groups(i, ks[:2], ks[2:])
            return
        core = me % 2
        (k0, d0), (k1, d1) = ((k, flipped(me, k)) for k in ks)
        for turn in range(2):
            swap = core if turn == 0 else 1 - core
            step_two_three(k0 + swap * (k1 - k0), i, d0 + swap * (d1 - d0))
            if turn == 0:
                pl.semaphore_wait(barrier, len(DIRECT))
            for x, k in enumerate(ks):
                @pl.when(swap == x)
                def _(k=k):
                    send(k, i)

    some(DIRECT[:2], 0, 0, True)
    some((*DIRECT[2:], 0, *DIAGONAL), 0, 0, False)

    def row(i, carry):
        slot = lax.rem(i, 2)
        fetch(i).wait()

        @pl.when(i + 1 < rows)
        def _():
            fetch(i + 1).start()

        def first(g, carry):
            q, t = step_one(slot, g, l1_ref[...])
            t1_ref[:, q, :] = t
            return carry

        lax.fori_loop(0, n // 16, first, 0)
        groups(i, DIRECT[:4], (*DIRECT[4:], 0, *DIAGONAL))
        return carry

    lax.fori_loop(1, rows, row, 0)
    pltpu.make_async_copy(g_ref.at[0], got[0], own_sem).wait()
    for k in DIAGONAL:
        for copy in tile_copies(k, pl.ds(0, rows)):
            copy.wait()
    for k in DIRECT:
        remote(k, g_ref.at[k], got[k]).wait()


def out_kernel(n_in, wide, *refs):
    l4_ref, out_ref = refs[n_in], refs[-1]
    rhs = jnp.concatenate([r[...].reshape(-1, wide) for r in refs[:n_in]], axis=0)
    out_ref[...] = dot(l4_ref[...], rhs).reshape(out_ref.shape)


def tail_kernel(n, n_in, a0, lane, lanes, parts, *refs):
    l4_ref, out_hbm, (v_ref, sem) = refs[n_in], refs[-3], refs[-2:]
    rhs = jnp.concatenate([r[...].reshape(-1, lanes) for r in refs[:n_in]], axis=0)
    size = n // parts
    copies = []
    for x in range(parts):
        i = pl.ds(x * size, size)
        v_ref[i] = dot(l4_ref[pl.ds(8 * size * x, 8 * size)], rhs).reshape(size, 8, lanes)
        copies.append(pltpu.make_async_copy(
            v_ref.at[i], out_hbm.at[i, pl.ds(a0, 8), pl.ds(lane, lanes)], sem.at[x]))
        copies[-1].start()
    for copy in copies:
        copy.wait()


def solution(mesh):
    n_dev = mesh.shape['dev']

    def transform(ao_rows, coeffs):
        rows = ao_rows.shape[0]
        n = coeffs.shape[0]
        wide = n * n // n_dev
        me_arr = jnp.full((1,), lax.axis_index('dev'), jnp.int32)
        smem = pl.BlockSpec(memory_space=pltpu.SMEM)
        vmem = pl.BlockSpec(memory_space=pltpu.VMEM)
        hbm = pl.BlockSpec(memory_space=pl.ANY)

        def const(shape):
            return pl.BlockSpec(shape, lambda *_: (0,) * len(shape))

        square, second = (8 * n, 8 * n), (512, 4 * n)
        n_got = n_dev - len(DIAGONAL)
        shapes = [(rows, n, wide)] * n_got
        shapes += [(rows, size, lanes) for _ in DIAGONAL for _, size, _, lanes in TILES]
        outs = pl.pallas_call(
            functools.partial(exchange_kernel, n, n_dev, rows),
            in_specs=[hbm, vmem],
            out_specs=[hbm] * len(shapes),
            out_shape=[jax.ShapeDtypeStruct(s, BF16) for s in shapes],
            scratch_shapes=[
                pltpu.VMEM((2, n, n, n), BF16), pltpu.VMEM((n, n, 128), BF16),
                pltpu.VMEM((n_dev, rows, n, wide), BF16), pltpu.VMEM(square, BF16),
                pltpu.VMEM(second, BF16), pltpu.VMEM((n, n), BF16),
                pltpu.SemaphoreType.DMA((2,)), pltpu.SemaphoreType.DMA((n // 16,)), pltpu.SemaphoreType.DMA,
                pltpu.SemaphoreType.DMA((len(shapes) - n_got,)),
                pltpu.SemaphoreType.DMA((n_dev,)), pltpu.SemaphoreType.DMA((n_dev,))],
            compiler_params=pltpu.CompilerParams(collective_id=0, has_side_effects=True),
            name='exchange',
        )(ao_rows, coeffs)
        got, tiles = outs[:n_got], outs[n_got:]
        moved = {}
        for t in range(len(TILES)):
            for x, k in enumerate(DIAGONAL):
                moved[k, t] = lax.ppermute(
                    tiles[x * len(TILES) + t], 'dev', [(i, i ^ k) for i in range(n_dev)])
        l4 = pl.pallas_call(
            functools.partial(last_kernel, n, rows),
            in_specs=[smem, vmem, hbm],
            out_specs=vmem,
            out_shape=jax.ShapeDtypeStruct(square, BF16),
            name='last',
        )(me_arr, coeffs, got[0])

        out = None
        for t_i, (a0, size, lane, lanes) in enumerate(TILES):
            ins, specs = [], []
            for k in range(n_dev):
                block, at = (moved[k, t_i], (0, 0)) if (k, t_i) in moved else (got[k], (a0, lane))
                ins.append(block)
                specs.append(pl.BlockSpec((pl.Element(rows), pl.Element(8), pl.Element(lanes)), lambda i, at=at: (0, pl.multiple_of(at[0] + 8 * i, 8), at[1])))
            n_in = len(ins)
            ins.append(l4)
            specs.append(const(square))
            if out is not None:
                ins.append(out)
                specs.append(hbm)
            alone = size == 8
            out = pl.pallas_call(
                functools.partial(tail_kernel, n, n_in, a0, lane, lanes, 4) if alone
                else functools.partial(out_kernel, n_in, lanes),
                grid=(size // 8,),
                in_specs=specs,
                out_specs=hbm if alone else pl.BlockSpec(
                    (pl.Element(n), pl.Element(8), pl.Element(lanes)),
                    lambda i, at=(a0, lane): (0, pl.multiple_of(at[0] + 8 * i, 8), at[1])),
                out_shape=jax.ShapeDtypeStruct((n, n, wide), F32),
                input_output_aliases={} if t_i == 0 else {len(ins) - 1: 0},
                scratch_shapes=[pltpu.VMEM((n, 8, lanes), F32), pltpu.SemaphoreType.DMA((4,))] * alone,
                compiler_params=pltpu.CompilerParams(vmem_limit_bytes=67043328),
                name='out',
            )(*ins)
        return out

    return jax.shard_map(transform, mesh=mesh, in_specs=(P(('frag', 'dev')), P('frag')), out_specs=P('frag', None, 'dev'), check_vma=False)
```

```python
import functools

import jax
import jax.numpy as jnp
from jax import lax
from jax.experimental import pallas as pl
from jax.experimental.pallas import tpu as pltpu
from jax.sharding import PartitionSpec as P


TILES = ((0, 48, 0, 1152), (48, 24, 0, 1152), (72, 8, 0, 1152), (80, 8, 0, 1152), (88, 8, 0, 640), (88, 8, 640, 512))
DIAGONAL = (6, 7)
DIRECT = (2, 4, 3, 5, 1)
F32, BF16 = jnp.float32, jnp.bfloat16


def one_hot(shape, fn):
    rows = lax.broadcasted_iota(jnp.int32, shape, 0)
    cols = lax.broadcasted_iota(jnp.int32, shape, 1)
    return fn(rows, cols)


def dot(a, b):
    return jnp.dot(a, b, preferred_element_type=F32)


def pick(shape, fn):
    return one_hot(shape, fn).astype(BF16)


def transposed(c, n):
    eye = pick((n, n), lambda i, j: i == j)
    return lax.dot_general(c, eye, (((0,), (0,)), ((), ())), preferred_element_type=F32).astype(BF16)


def build_first(n, c_ref, l1_ref, r2_ref, ct_ref):
    c = c_ref[...]
    ct = transposed(c, n)
    ct_ref[...] = ct
    tall = dot(pick((8 * n, n), lambda i, j: i // 8 == j), ct).astype(BF16)
    wide = dot(tall, pick((n, 8 * n), lambda i, j: j % n == i))
    keep = one_hot((8 * n, 8 * n), lambda i, j: i % 8 == j // n)
    l1_ref[...] = jnp.where(keep, wide, 0.0).astype(BF16)
    tall = dot(pick((512, n), lambda i, j: i % 128 == j), c).astype(BF16)
    wide = dot(tall, pick((n, 4 * n), lambda i, j: j % n == i))
    keep = one_hot((512, 4 * n), lambda i, j: i // 128 == j // n)
    r2_ref[...] = jnp.where(keep, wide, 0.0).astype(BF16)


def last_kernel(n, rows, me_ref, c_ref, after_ref, l4_ref):
    me = me_ref[0]

    def source(r, col):
        m = col // 8
        return r == (me ^ (m // rows)) * rows + m % rows

    ct = transposed(c_ref[...], n)
    tall = dot(pick((8 * n, n), lambda i, j: i // 8 == j), ct).astype(BF16)
    wide = dot(tall, pick((n, 8 * n), source))
    keep = one_hot((8 * n, 8 * n), lambda i, j: i % 8 == j % 8)
    l4_ref[...] = jnp.where(keep, wide, 0.0).astype(BF16)


def flipped(me, k):
    out = 0
    for bit in (1, 2, 4):
        b = (me // bit) % 2
        out = out + bit * (1 - b if k & bit else b)
    return out


def exchange_kernel(n, n_dev, rows, a_hbm, c_ref, *refs):
    n_got, n_tile = n_dev - len(DIAGONAL), len(TILES)
    got, tiles = refs[:n_got], refs[n_got:n_got + len(DIAGONAL) * n_tile]
    (a_buf, t1_ref, g_ref, l1_ref, r2_ref, ct_ref, a_sem, chunk_sem, own_sem, tile_sem, send_sem,
     recv_sem) = refs[n_got + len(tiles):]
    nj = n // n_dev
    me = lax.axis_index('dev')
    barrier = pltpu.get_barrier_semaphore()
    for k in DIRECT:
        pl.semaphore_signal(barrier, inc=1, device_id={'dev': flipped(me, k)}, device_id_type=pl.DeviceIdType.MESH)

    def chunk(g):
        q = pl.ds(g * 16, 16)
        return pltpu.make_async_copy(a_hbm.at[0, q], a_buf.at[0, q], chunk_sem.at[g])

    def fetch(i):
        slot = lax.rem(i, 2)
        return pltpu.make_async_copy(a_hbm.at[i], a_buf.at[slot], a_sem.at[slot])

    for g in range(n // 16):
        chunk(g).start()
    fetch(1).start()
    build_first(n, c_ref, l1_ref, r2_ref, ct_ref)
    zero = jnp.zeros((8 * n, 128 - n), BF16)

    def remote(k, src, dst):
        return pltpu.make_async_remote_copy(
            src_ref=src, dst_ref=dst, send_sem=send_sem.at[k], recv_sem=recv_sem.at[k],
            device_id={'dev': flipped(me, k)}, device_id_type=pl.DeviceIdType.MESH)

    def tile_copies(k, rows_):
        x = DIAGONAL.index(k)
        for t, (a0, size, lane, lanes) in enumerate(TILES):
            j = x * n_tile + t
            src = g_ref.at[k, rows_, pl.ds(a0, size), pl.ds(lane, lanes)]
            yield pltpu.make_async_copy(src, tiles[j].at[rows_], tile_sem.at[j])

    def send(k, i):
        if k == 0:
            pltpu.make_async_copy(g_ref.at[0, i], got[0].at[i], own_sem).start()
        elif k in DIAGONAL:
            for copy in tile_copies(k, i):
                copy.start()
        else:
            remote(k, g_ref.at[k, i], got[k].at[i]).start()

    def step_one(slot, g, lhs):
        q0 = pl.multiple_of(g * 16, 16)
        lo = a_buf[slot, pl.ds(q0, 8)].reshape(8 * n, n)
        hi = a_buf[slot, pl.ds(q0 + 8, 8)].reshape(8 * n, n)
        t = dot(lhs, jnp.concatenate([lo, zero, hi, zero], axis=1))
        nj = t.shape[0] // 8
        t = jnp.concatenate([t[:, :128].reshape(nj, 8, 128), t[:, 128:].reshape(nj, 8, 128)], axis=1)
        return pl.ds(q0, 16), t.astype(BF16)

    def step_two_three(k, i):
        d = flipped(me, k)
        t = t1_ref[pl.ds(d * nj, nj)].reshape(nj // 4, 4, n, 128)
        lhs = jnp.concatenate([t[:, jj].reshape(nj // 4 * n, 128) for jj in range(4)], axis=1)
        h = dot(lhs, r2_ref[...]).astype(BF16)
        h = jnp.concatenate([h[g * n:(g + 1) * n] for g in range(nj // 4)], axis=1)
        g_ref[k, i] = dot(ct_ref[...], h).astype(BF16)

    def some(ks, i, slot, wait):
        def first(pair, carry):
            if wait:
                chunk(2 * pair).wait()
                chunk(2 * pair + 1).wait()
            lhs = jnp.concatenate(
                [l1_ref[pl.ds(pl.multiple_of(flipped(me, k) * 8 * nj, 8 * nj), 8 * nj)] for k in ks], axis=0)
            for g in range(2):
                q, t = step_one(slot, 2 * pair + g, lhs)
                for x, k in enumerate(ks):
                    t1_ref[pl.ds(flipped(me, k) * nj, nj), q, :] = t[x * nj:(x + 1) * nj]
            return carry

        lax.fori_loop(0, n // 32, first, 0)
        for k in ks:
            step_two_three(k, i)
        if wait:
            pl.semaphore_wait(barrier, len(DIRECT))
        for k in ks:
            send(k, i)

    some(DIRECT[:2], 0, 0, True)
    some((*DIRECT[2:], 0, *DIAGONAL), 0, 0, False)

    def row(i, carry):
        slot = lax.rem(i, 2)
        fetch(i).wait()

        @pl.when(i + 1 < rows)
        def _():
            fetch(i + 1).start()

        def first(g, carry):
            q, t = step_one(slot, g, l1_ref[...])
            t1_ref[:, q, :] = t
            return carry

        lax.fori_loop(0, n // 16, first, 0)
        before = None
        for k in (*DIRECT, 0, *DIAGONAL):
            step_two_three(k, i)
            if before is not None:
                send(before, i)
            before = k
        send(before, i)
        return carry

    lax.fori_loop(1, rows, row, 0)
    pltpu.make_async_copy(g_ref.at[0], got[0], own_sem).wait()
    for k in DIAGONAL:
        for copy in tile_copies(k, pl.ds(0, rows)):
            copy.wait()
    for k in DIRECT:
        remote(k, g_ref.at[k], got[k]).wait()


def out_kernel(n_in, wide, *refs):
    l4_ref, out_ref = refs[n_in], refs[-1]
    rhs = jnp.concatenate([r[...].reshape(-1, wide) for r in refs[:n_in]], axis=0)
    out_ref[...] = dot(l4_ref[...], rhs).reshape(out_ref.shape)


def tail_kernel(n, n_in, a0, lane, lanes, parts, *refs):
    l4_ref, out_hbm, (v_ref, sem) = refs[n_in], refs[-3], refs[-2:]
    rhs = jnp.concatenate([r[...].reshape(-1, lanes) for r in refs[:n_in]], axis=0)
    size = n // parts
    copies = []
    for x in range(parts):
        i = pl.ds(x * size, size)
        v_ref[i] = dot(l4_ref[pl.ds(8 * size * x, 8 * size)], rhs).reshape(size, 8, lanes)
        copies.append(pltpu.make_async_copy(
            v_ref.at[i], out_hbm.at[i, pl.ds(a0, 8), pl.ds(lane, lanes)], sem.at[x]))
        copies[-1].start()
    for copy in copies:
        copy.wait()


def solution(mesh):
    n_dev = mesh.shape['dev']

    def transform(ao_rows, coeffs):
        rows = ao_rows.shape[0]
        n = coeffs.shape[0]
        wide = n * n // n_dev
        me_arr = jnp.full((1,), lax.axis_index('dev'), jnp.int32)
        smem = pl.BlockSpec(memory_space=pltpu.SMEM)
        vmem = pl.BlockSpec(memory_space=pltpu.VMEM)
        hbm = pl.BlockSpec(memory_space=pl.ANY)

        def const(shape):
            return pl.BlockSpec(shape, lambda *_: (0,) * len(shape))

        square, second = (8 * n, 8 * n), (512, 4 * n)
        n_got = n_dev - len(DIAGONAL)
        shapes = [(rows, n, wide)] * n_got
        shapes += [(rows, size, lanes) for _ in DIAGONAL for _, size, _, lanes in TILES]
        outs = pl.pallas_call(
            functools.partial(exchange_kernel, n, n_dev, rows),
            in_specs=[hbm, vmem],
            out_specs=[hbm] * len(shapes),
            out_shape=[jax.ShapeDtypeStruct(s, BF16) for s in shapes],
            scratch_shapes=[
                pltpu.VMEM((2, n, n, n), BF16), pltpu.VMEM((n, n, 128), BF16),
                pltpu.VMEM((n_dev, rows, n, wide), BF16), pltpu.VMEM(square, BF16),
                pltpu.VMEM(second, BF16), pltpu.VMEM((n, n), BF16),
                pltpu.SemaphoreType.DMA((2,)), pltpu.SemaphoreType.DMA((n // 16,)), pltpu.SemaphoreType.DMA,
                pltpu.SemaphoreType.DMA((len(shapes) - n_got,)),
                pltpu.SemaphoreType.DMA((n_dev,)), pltpu.SemaphoreType.DMA((n_dev,))],
            compiler_params=pltpu.CompilerParams(collective_id=0, has_side_effects=True),
            name='exchange',
        )(ao_rows, coeffs)
        got, tiles = outs[:n_got], outs[n_got:]
        moved = {}
        for t in range(len(TILES)):
            for x, k in enumerate(DIAGONAL):
                moved[k, t] = lax.ppermute(
                    tiles[x * len(TILES) + t], 'dev', [(i, i ^ k) for i in range(n_dev)])
        l4 = pl.pallas_call(
            functools.partial(last_kernel, n, rows),
            in_specs=[smem, vmem, hbm],
            out_specs=vmem,
            out_shape=jax.ShapeDtypeStruct(square, BF16),
            name='last',
        )(me_arr, coeffs, got[0])

        out = None
        for t_i, (a0, size, lane, lanes) in enumerate(TILES):
            ins, specs = [], []
            for k in range(n_dev):
                block, at = (moved[k, t_i], (0, 0)) if (k, t_i) in moved else (got[k], (a0, lane))
                ins.append(block)
                specs.append(pl.BlockSpec((pl.Element(rows), pl.Element(8), pl.Element(lanes)), lambda i, at=at: (0, pl.multiple_of(at[0] + 8 * i, 8), at[1])))
            n_in = len(ins)
            ins.append(l4)
            specs.append(const(square))
            if out is not None:
                ins.append(out)
                specs.append(hbm)
            alone = size == 8
            out = pl.pallas_call(
                functools.partial(tail_kernel, n, n_in, a0, lane, lanes, 4) if alone
                else functools.partial(out_kernel, n_in, lanes),
                grid=(size // 8,),
                in_specs=specs,
                out_specs=hbm if alone else pl.BlockSpec(
                    (pl.Element(n), pl.Element(8), pl.Element(lanes)),
                    lambda i, at=(a0, lane): (0, pl.multiple_of(at[0] + 8 * i, 8), at[1])),
                out_shape=jax.ShapeDtypeStruct((n, n, wide), F32),
                input_output_aliases={} if t_i == 0 else {len(ins) - 1: 0},
                scratch_shapes=[pltpu.VMEM((n, 8, lanes), F32), pltpu.SemaphoreType.DMA((4,))] * alone,
                compiler_params=pltpu.CompilerParams(vmem_limit_bytes=67043328),
                name='out',
            )(*ins)
        return out

    return jax.shard_map(transform, mesh=mesh, in_specs=(P(('frag', 'dev')), P('frag')), out_specs=P('frag', None, 'dev'), check_vma=False)
```

```python
import functools

import jax
import jax.numpy as jnp
from jax import lax
from jax.experimental import pallas as pl
from jax.experimental.pallas import tpu as pltpu
from jax.sharding import PartitionSpec as P


TILES = ((0, 48, 0, 1152), (48, 24, 0, 1152), (72, 8, 0, 1152), (80, 8, 0, 1152), (88, 8, 0, 640), (88, 8, 640, 512))
DIAGONAL = (6, 7)
DIRECT = (4, 2, 5, 3, 1)
F32, BF16 = jnp.float32, jnp.bfloat16


def one_hot(shape, fn):
    rows = lax.broadcasted_iota(jnp.int32, shape, 0)
    cols = lax.broadcasted_iota(jnp.int32, shape, 1)
    return fn(rows, cols)


def dot(a, b):
    return jnp.dot(a, b, preferred_element_type=F32)


def pick(shape, fn):
    return one_hot(shape, fn).astype(BF16)


def transposed(c, n):
    eye = pick((n, n), lambda i, j: i == j)
    return lax.dot_general(c, eye, (((0,), (0,)), ((), ())), preferred_element_type=F32).astype(BF16)


def l1_rows(n, j_of, size, ct):
    tall = dot(pick((8 * size, n), lambda i, j: j_of(i // 8) == j), ct).astype(BF16)
    wide = dot(tall, pick((n, 8 * n), lambda i, j: j % n == i))
    keep = one_hot((8 * size, 8 * n), lambda i, j: i % 8 == j // n)
    return jnp.where(keep, wide, 0.0).astype(BF16)


def build_first(n, j_of, size, c_ref, l1_ref, r2_ref, ct_ref):
    c = c_ref[...]
    ct = transposed(c, n)
    ct_ref[...] = ct
    l1_ref[pl.ds(0, 8 * size)] = l1_rows(n, j_of, size, ct)
    tall = dot(pick((512, n), lambda i, j: i % 128 == j), c).astype(BF16)
    wide = dot(tall, pick((n, 4 * n), lambda i, j: j % n == i))
    keep = one_hot((512, 4 * n), lambda i, j: i // 128 == j // n)
    r2_ref[...] = jnp.where(keep, wide, 0.0).astype(BF16)


def last_kernel(n, rows, me_ref, c_ref, after_ref, l4_ref):
    me = me_ref[0]

    def source(r, col):
        m = col // 8
        return r == (me ^ (m // rows)) * rows + m % rows

    ct = transposed(c_ref[...], n)
    tall = dot(pick((8 * n, n), lambda i, j: i // 8 == j), ct).astype(BF16)
    wide = dot(tall, pick((n, 8 * n), source))
    keep = one_hot((8 * n, 8 * n), lambda i, j: i % 8 == j % 8)
    l4_ref[...] = jnp.where(keep, wide, 0.0).astype(BF16)


def flipped(me, k):
    out = 0
    for bit in (1, 2, 4):
        b = (me // bit) % 2
        out = out + bit * (1 - b if k & bit else b)
    return out


def exchange_kernel(n, n_dev, rows, a_hbm, c_ref, *refs):
    n_got, n_tile = n_dev - len(DIAGONAL), len(TILES)
    got, tiles = refs[:n_got], refs[n_got:n_got + len(DIAGONAL) * n_tile]
    (a_buf, t1_ref, g_ref, l1_ref, r2_ref, ct_ref, a_sem, chunk_sem, own_sem, tile_sem, send_sem,
     recv_sem) = refs[n_got + len(tiles):]
    nj = n // n_dev
    me = lax.axis_index('dev')
    barrier = pltpu.get_barrier_semaphore()
    for k in DIRECT:
        pl.semaphore_signal(barrier, inc=1, device_id={'dev': flipped(me, k)}, device_id_type=pl.DeviceIdType.MESH)

    def chunk(g):
        q = pl.ds(g * 16, 16)
        return pltpu.make_async_copy(a_hbm.at[0, q], a_buf.at[0, q], chunk_sem.at[g])

    def fetch(i):
        slot = lax.rem(i, 2)
        return pltpu.make_async_copy(a_hbm.at[i], a_buf.at[slot], a_sem.at[slot])

    for g in range(n // 16):
        chunk(g).start()
    fetch(1).start()
    d0, d1 = (flipped(me, k) for k in DIRECT[:2])
    build_first(n, lambda x: jnp.where(x < nj, x + d0 * nj, x - nj + d1 * nj), 2 * nj, c_ref, l1_ref, r2_ref, ct_ref)
    zero = jnp.zeros((8 * n, 128 - n), BF16)

    def remote(k, src, dst):
        return pltpu.make_async_remote_copy(
            src_ref=src, dst_ref=dst, send_sem=send_sem.at[k], recv_sem=recv_sem.at[k],
            device_id={'dev': flipped(me, k)}, device_id_type=pl.DeviceIdType.MESH)

    def tile_copies(k, rows_):
        x = DIAGONAL.index(k)
        for t, (a0, size, lane, lanes) in enumerate(TILES):
            j = x * n_tile + t
            src = g_ref.at[k, rows_, pl.ds(a0, size), pl.ds(lane, lanes)]
            yield pltpu.make_async_copy(src, tiles[j].at[rows_], tile_sem.at[j])

    def send(k, i):
        if k == 0:
            pltpu.make_async_copy(g_ref.at[0, i], got[0].at[i], own_sem).start()
        elif k in DIAGONAL:
            for copy in tile_copies(k, i):
                copy.start()
        else:
            remote(k, g_ref.at[k, i], got[k].at[i]).start()

    def step_one(slot, g, lhs):
        q0 = pl.multiple_of(g * 16, 16)
        lo = a_buf[slot, pl.ds(q0, 8)].reshape(8 * n, n)
        hi = a_buf[slot, pl.ds(q0 + 8, 8)].reshape(8 * n, n)
        t = dot(lhs, jnp.concatenate([lo, zero, hi, zero], axis=1))
        nj = t.shape[0] // 8
        t = jnp.concatenate([t[:, :128].reshape(nj, 8, 128), t[:, 128:].reshape(nj, 8, 128)], axis=1)
        return pl.ds(q0, 16), t.astype(BF16)

    def step_two_three(k, i):
        d = flipped(me, k)
        t = t1_ref[pl.ds(d * nj, nj)].reshape(nj // 4, 4, n, 128)
        lhs = jnp.concatenate([t[:, jj].reshape(nj // 4 * n, 128) for jj in range(4)], axis=1)
        h = dot(lhs, r2_ref[...]).astype(BF16)
        h = jnp.concatenate([h[g * n:(g + 1) * n] for g in range(nj // 4)], axis=1)
        g_ref[k, i] = dot(ct_ref[...], h).astype(BF16)

    def some(ks, i, slot, wait):
        def first(pair, carry):
            if wait:
                chunk(2 * pair).wait()
                chunk(2 * pair + 1).wait()
                lhs = l1_ref[pl.ds(0, len(ks) * 8 * nj)]
            else:
                lhs = jnp.concatenate(
                    [l1_ref[pl.ds(pl.multiple_of(flipped(me, k) * 8 * nj, 8 * nj), 8 * nj)] for k in ks], axis=0)
            for g in range(2):
                q, t = step_one(slot, 2 * pair + g, lhs)
                for x, k in enumerate(ks):
                    t1_ref[pl.ds(flipped(me, k) * nj, nj), q, :] = t[x * nj:(x + 1) * nj]
            return carry

        lax.fori_loop(0, n // 32, first, 0)
        for part in (ks,) if wait else (ks[:2], ks[2:]):
            for k in part:
                step_two_three(k, i)
            if wait:
                pl.semaphore_wait(barrier, len(DIRECT))
            for k in part:
                send(k, i)

    some(DIRECT[:2], 0, 0, True)
    l1_ref[...] = l1_rows(n, lambda x: x, n, ct_ref[...])
    some((*DIRECT[2:], 0, *DIAGONAL), 0, 0, False)

    def row(i, carry):
        slot = lax.rem(i, 2)
        fetch(i).wait()

        @pl.when(i + 1 < rows)
        def _():
            fetch(i + 1).start()

        def first(g, carry):
            q, t = step_one(slot, g, l1_ref[...])
            t1_ref[:, q, :] = t
            return carry

        lax.fori_loop(0, n // 16, first, 0)
        before = None
        for k in (*DIRECT, 0, *DIAGONAL):
            step_two_three(k, i)
            if before is not None:
                send(before, i)
            before = k
        send(before, i)
        return carry

    lax.fori_loop(1, rows, row, 0)
    pltpu.make_async_copy(g_ref.at[0], got[0], own_sem).wait()
    for k in DIAGONAL:
        for copy in tile_copies(k, pl.ds(0, rows)):
            copy.wait()
    for k in DIRECT:
        remote(k, g_ref.at[k], got[k]).wait()


def out_kernel(n_in, wide, *refs):
    l4_ref, out_ref = refs[n_in], refs[-1]
    rhs = jnp.concatenate([r[...].reshape(-1, wide) for r in refs[:n_in]], axis=0)
    out_ref[...] = dot(l4_ref[...], rhs).reshape(out_ref.shape)


def tail_kernel(n, n_in, a0, lane, lanes, parts, *refs):
    l4_ref, out_hbm, (v_ref, sem) = refs[n_in], refs[-3], refs[-2:]
    rhs = jnp.concatenate([r[...].reshape(-1, lanes) for r in refs[:n_in]], axis=0)
    size = n // parts
    copies = []
    for x in range(parts):
        i = pl.ds(x * size, size)
        v_ref[i] = dot(l4_ref[pl.ds(8 * size * x, 8 * size)], rhs).reshape(size, 8, lanes)
        copies.append(pltpu.make_async_copy(
            v_ref.at[i], out_hbm.at[i, pl.ds(a0, 8), pl.ds(lane, lanes)], sem.at[x]))
        copies[-1].start()
    for copy in copies:
        copy.wait()


def solution(mesh):
    n_dev = mesh.shape['dev']

    def transform(ao_rows, coeffs):
        rows = ao_rows.shape[0]
        n = coeffs.shape[0]
        wide = n * n // n_dev
        me_arr = jnp.full((1,), lax.axis_index('dev'), jnp.int32)
        smem = pl.BlockSpec(memory_space=pltpu.SMEM)
        vmem = pl.BlockSpec(memory_space=pltpu.VMEM)
        hbm = pl.BlockSpec(memory_space=pl.ANY)

        def const(shape):
            return pl.BlockSpec(shape, lambda *_: (0,) * len(shape))

        square, second = (8 * n, 8 * n), (512, 4 * n)
        n_got = n_dev - len(DIAGONAL)
        shapes = [(rows, n, wide)] * n_got
        shapes += [(rows, size, lanes) for _ in DIAGONAL for _, size, _, lanes in TILES]
        outs = pl.pallas_call(
            functools.partial(exchange_kernel, n, n_dev, rows),
            in_specs=[hbm, vmem],
            out_specs=[hbm] * len(shapes),
            out_shape=[jax.ShapeDtypeStruct(s, BF16) for s in shapes],
            scratch_shapes=[
                pltpu.VMEM((2, n, n, n), BF16), pltpu.VMEM((n, n, 128), BF16),
                pltpu.VMEM((n_dev, rows, n, wide), BF16), pltpu.VMEM(square, BF16),
                pltpu.VMEM(second, BF16), pltpu.VMEM((n, n), BF16),
                pltpu.SemaphoreType.DMA((2,)), pltpu.SemaphoreType.DMA((n // 16,)), pltpu.SemaphoreType.DMA,
                pltpu.SemaphoreType.DMA((len(shapes) - n_got,)),
                pltpu.SemaphoreType.DMA((n_dev,)), pltpu.SemaphoreType.DMA((n_dev,))],
            compiler_params=pltpu.CompilerParams(collective_id=0, has_side_effects=True),
            name='exchange',
        )(ao_rows, coeffs)
        got, tiles = outs[:n_got], outs[n_got:]
        moved = {}
        for t in range(len(TILES)):
            for x, k in enumerate(DIAGONAL):
                moved[k, t] = lax.ppermute(
                    tiles[x * len(TILES) + t], 'dev', [(i, i ^ k) for i in range(n_dev)])
        l4 = pl.pallas_call(
            functools.partial(last_kernel, n, rows),
            in_specs=[smem, vmem, hbm],
            out_specs=vmem,
            out_shape=jax.ShapeDtypeStruct(square, BF16),
            name='last',
        )(me_arr, coeffs, got[0])

        out = None
        for t_i, (a0, size, lane, lanes) in enumerate(TILES):
            ins, specs = [], []
            for k in range(n_dev):
                block, at = (moved[k, t_i], (0, 0)) if (k, t_i) in moved else (got[k], (a0, lane))
                ins.append(block)
                specs.append(pl.BlockSpec((pl.Element(rows), pl.Element(8), pl.Element(lanes)), lambda i, at=at: (0, pl.multiple_of(at[0] + 8 * i, 8), at[1])))
            n_in = len(ins)
            ins.append(l4)
            specs.append(const(square))
            if out is not None:
                ins.append(out)
                specs.append(hbm)
            alone = size == 8
            out = pl.pallas_call(
                functools.partial(tail_kernel, n, n_in, a0, lane, lanes, 4) if alone
                else functools.partial(out_kernel, n_in, lanes),
                grid=(size // 8,),
                in_specs=specs,
                out_specs=hbm if alone else pl.BlockSpec(
                    (pl.Element(n), pl.Element(8), pl.Element(lanes)),
                    lambda i, at=(a0, lane): (0, pl.multiple_of(at[0] + 8 * i, 8), at[1])),
                out_shape=jax.ShapeDtypeStruct((n, n, wide), F32),
                input_output_aliases={} if t_i == 0 else {len(ins) - 1: 0},
                scratch_shapes=[pltpu.VMEM((n, 8, lanes), F32), pltpu.SemaphoreType.DMA((4,))] * alone,
                compiler_params=pltpu.CompilerParams(vmem_limit_bytes=67043328),
                name='out',
            )(*ins)
        return out

    return jax.shard_map(transform, mesh=mesh, in_specs=(P(('frag', 'dev')), P('frag')), out_specs=P('frag', None, 'dev'), check_vma=False)
```

```python
import functools

import jax
import jax.numpy as jnp
from jax import lax
from jax.experimental import pallas as pl
from jax.experimental.pallas import tpu as pltpu
from jax.sharding import PartitionSpec as P


TILES = ((0, 48, 0, 1152), (48, 24, 0, 1152), (72, 8, 0, 1152), (80, 8, 0, 1152), (88, 8, 0, 640), (88, 8, 640, 512))
DIAGONAL = (6, 7)
DIRECT = (2, 4, 3, 5, 1)
F32, BF16 = jnp.float32, jnp.bfloat16


def one_hot(shape, fn):
    rows = lax.broadcasted_iota(jnp.int32, shape, 0)
    cols = lax.broadcasted_iota(jnp.int32, shape, 1)
    return fn(rows, cols)


def dot(a, b):
    return jnp.dot(a, b, preferred_element_type=F32)


def pick(shape, fn):
    return one_hot(shape, fn).astype(BF16)


def transposed(c, n):
    eye = pick((n, n), lambda i, j: i == j)
    return lax.dot_general(c, eye, (((0,), (0,)), ((), ())), preferred_element_type=F32).astype(BF16)


def l1_rows(n, j_of, size, ct):
    tall = dot(pick((8 * size, n), lambda i, j: j_of(i // 8) == j), ct).astype(BF16)
    wide = dot(tall, pick((n, 8 * n), lambda i, j: j % n == i))
    keep = one_hot((8 * size, 8 * n), lambda i, j: i % 8 == j // n)
    return jnp.where(keep, wide, 0.0).astype(BF16)


def build_first(n, j_of, size, c_ref, l1_ref, r2_ref, ct_ref):
    c = c_ref[...]
    ct = transposed(c, n)
    ct_ref[...] = ct
    l1_ref[pl.ds(0, 8 * size)] = l1_rows(n, j_of, size, ct)
    tall = dot(pick((512, n), lambda i, j: i % 128 == j), c).astype(BF16)
    wide = dot(tall, pick((n, 4 * n), lambda i, j: j % n == i))
    keep = one_hot((512, 4 * n), lambda i, j: i // 128 == j // n)
    r2_ref[...] = jnp.where(keep, wide, 0.0).astype(BF16)


def last_kernel(n, rows, me_ref, c_ref, after_ref, l4_ref):
    me = me_ref[0]

    def source(r, col):
        m = col // 8
        return r == (me ^ (m // rows)) * rows + m % rows

    ct = transposed(c_ref[...], n)
    tall = dot(pick((8 * n, n), lambda i, j: i // 8 == j), ct).astype(BF16)
    wide = dot(tall, pick((n, 8 * n), source))
    keep = one_hot((8 * n, 8 * n), lambda i, j: i % 8 == j % 8)
    l4_ref[...] = jnp.where(keep, wide, 0.0).astype(BF16)


def flipped(me, k):
    out = 0
    for bit in (1, 2, 4):
        b = (me // bit) % 2
        out = out + bit * (1 - b if k & bit else b)
    return out


def exchange_kernel(n, n_dev, rows, a_hbm, c_ref, *refs):
    n_got, n_tile = n_dev - len(DIAGONAL), len(TILES)
    got, tiles = refs[:n_got], refs[n_got:n_got + len(DIAGONAL) * n_tile]
    (a_buf, t1_ref, g_ref, l1_ref, r2_ref, ct_ref, a_sem, chunk_sem, own_sem, tile_sem, send_sem,
     recv_sem) = refs[n_got + len(tiles):]
    nj = n // n_dev
    me = lax.axis_index('dev')
    barrier = pltpu.get_barrier_semaphore()
    for k in DIRECT:
        pl.semaphore_signal(barrier, inc=1, device_id={'dev': flipped(me, k)}, device_id_type=pl.DeviceIdType.MESH)

    def chunk(g):
        q = pl.ds(g * 16, 16)
        return pltpu.make_async_copy(a_hbm.at[0, q], a_buf.at[0, q], chunk_sem.at[g])

    def fetch(i):
        slot = lax.rem(i, 2)
        return pltpu.make_async_copy(a_hbm.at[i], a_buf.at[slot], a_sem.at[slot])

    for g in range(n // 16):
        chunk(g).start()
    fetch(1).start()
    d0, d1 = (flipped(me, k) for k in DIRECT[:2])
    build_first(n, lambda x: jnp.where(x < nj, x + d0 * nj, x - nj + d1 * nj), 2 * nj, c_ref, l1_ref, r2_ref, ct_ref)
    zero = jnp.zeros((8 * n, 128 - n), BF16)

    def remote(k, src, dst):
        return pltpu.make_async_remote_copy(
            src_ref=src, dst_ref=dst, send_sem=send_sem.at[k], recv_sem=recv_sem.at[k],
            device_id={'dev': flipped(me, k)}, device_id_type=pl.DeviceIdType.MESH)

    def tile_copies(k, rows_):
        x = DIAGONAL.index(k)
        for t, (a0, size, lane, lanes) in enumerate(TILES):
            j = x * n_tile + t
            src = g_ref.at[k, rows_, pl.ds(a0, size), pl.ds(lane, lanes)]
            yield pltpu.make_async_copy(src, tiles[j].at[rows_], tile_sem.at[j])

    def send(k, i):
        if k == 0:
            pltpu.make_async_copy(g_ref.at[0, i], got[0].at[i], own_sem).start()
        elif k in DIAGONAL:
            for copy in tile_copies(k, i):
                copy.start()
        else:
            remote(k, g_ref.at[k, i], got[k].at[i]).start()

    def step_one(slot, g, lhs):
        q0 = pl.multiple_of(g * 16, 16)
        lo = a_buf[slot, pl.ds(q0, 8)].reshape(8 * n, n)
        hi = a_buf[slot, pl.ds(q0 + 8, 8)].reshape(8 * n, n)
        t = dot(lhs, jnp.concatenate([lo, zero, hi, zero], axis=1))
        nj = t.shape[0] // 8
        t = jnp.concatenate([t[:, :128].reshape(nj, 8, 128), t[:, 128:].reshape(nj, 8, 128)], axis=1)
        return pl.ds(q0, 16), t.astype(BF16)

    def step_two_three(k, i):
        d = flipped(me, k)
        t = t1_ref[pl.ds(d * nj, nj)].reshape(nj // 4, 4, n, 128)
        lhs = jnp.concatenate([t[:, jj].reshape(nj // 4 * n, 128) for jj in range(4)], axis=1)
        h = dot(lhs, r2_ref[...]).astype(BF16)
        h = jnp.concatenate([h[g * n:(g + 1) * n] for g in range(nj // 4)], axis=1)
        g_ref[k, i] = dot(ct_ref[...], h).astype(BF16)

    def some(ks, i, slot, wait):
        def first(pair, carry):
            if wait:
                chunk(2 * pair).wait()
                chunk(2 * pair + 1).wait()
                lhs = l1_ref[pl.ds(0, len(ks) * 8 * nj)]
            else:
                lhs = jnp.concatenate(
                    [l1_ref[pl.ds(pl.multiple_of(flipped(me, k) * 8 * nj, 8 * nj), 8 * nj)] for k in ks], axis=0)
            for g in range(2):
                q, t = step_one(slot, 2 * pair + g, lhs)
                for x, k in enumerate(ks):
                    t1_ref[pl.ds(flipped(me, k) * nj, nj), q, :] = t[x * nj:(x + 1) * nj]
            return carry

        lax.fori_loop(0, n // 32, first, 0)
        for part in (ks,) if wait else (ks[:2], ks[2:]):
            for k in part:
                step_two_three(k, i)
            if wait:
                pl.semaphore_wait(barrier, len(DIRECT))
            for k in part:
                send(k, i)

    some(DIRECT[:2], 0, 0, True)
    l1_ref[...] = l1_rows(n, lambda x: x, n, ct_ref[...])
    some((*DIRECT[2:], 0, *DIAGONAL), 0, 0, False)

    def row(i, carry):
        slot = lax.rem(i, 2)
        fetch(i).wait()

        @pl.when(i + 1 < rows)
        def _():
            fetch(i + 1).start()

        def first(g, carry):
            q, t = step_one(slot, g, l1_ref[...])
            t1_ref[:, q, :] = t
            return carry

        lax.fori_loop(0, n // 16, first, 0)
        before = None
        for k in (*DIRECT, 0, *DIAGONAL):
            step_two_three(k, i)
            if before is not None:
                send(before, i)
            before = k
        send(before, i)
        return carry

    lax.fori_loop(1, rows, row, 0)
    pltpu.make_async_copy(g_ref.at[0], got[0], own_sem).wait()
    for k in DIAGONAL:
        for copy in tile_copies(k, pl.ds(0, rows)):
            copy.wait()
    for k in DIRECT:
        remote(k, g_ref.at[k], got[k]).wait()


def out_kernel(n_in, wide, *refs):
    l4_ref, out_ref = refs[n_in], refs[-1]
    rhs = jnp.concatenate([r[...].reshape(-1, wide) for r in refs[:n_in]], axis=0)
    out_ref[...] = dot(l4_ref[...], rhs).reshape(out_ref.shape)


def tail_kernel(n, n_in, a0, lane, lanes, parts, *refs):
    l4_ref, out_hbm, (v_ref, sem) = refs[n_in], refs[-3], refs[-2:]
    rhs = jnp.concatenate([r[...].reshape(-1, lanes) for r in refs[:n_in]], axis=0)
    size = n // parts
    copies = []
    for x in range(parts):
        i = pl.ds(x * size, size)
        v_ref[i] = dot(l4_ref[pl.ds(8 * size * x, 8 * size)], rhs).reshape(size, 8, lanes)
        copies.append(pltpu.make_async_copy(
            v_ref.at[i], out_hbm.at[i, pl.ds(a0, 8), pl.ds(lane, lanes)], sem.at[x]))
        copies[-1].start()
    for copy in copies:
        copy.wait()


def solution(mesh):
    n_dev = mesh.shape['dev']

    def transform(ao_rows, coeffs):
        rows = ao_rows.shape[0]
        n = coeffs.shape[0]
        wide = n * n // n_dev
        me_arr = jnp.full((1,), lax.axis_index('dev'), jnp.int32)
        smem = pl.BlockSpec(memory_space=pltpu.SMEM)
        vmem = pl.BlockSpec(memory_space=pltpu.VMEM)
        hbm = pl.BlockSpec(memory_space=pl.ANY)

        def const(shape):
            return pl.BlockSpec(shape, lambda *_: (0,) * len(shape))

        square, second = (8 * n, 8 * n), (512, 4 * n)
        n_got = n_dev - len(DIAGONAL)
        shapes = [(rows, n, wide)] * n_got
        shapes += [(rows, size, lanes) for _ in DIAGONAL for _, size, _, lanes in TILES]
        outs = pl.pallas_call(
            functools.partial(exchange_kernel, n, n_dev, rows),
            in_specs=[hbm, vmem],
            out_specs=[hbm] * len(shapes),
            out_shape=[jax.ShapeDtypeStruct(s, BF16) for s in shapes],
            scratch_shapes=[
                pltpu.VMEM((2, n, n, n), BF16), pltpu.VMEM((n, n, 128), BF16),
                pltpu.VMEM((n_dev, rows, n, wide), BF16), pltpu.VMEM(square, BF16),
                pltpu.VMEM(second, BF16), pltpu.VMEM((n, n), BF16),
                pltpu.SemaphoreType.DMA((2,)), pltpu.SemaphoreType.DMA((n // 16,)), pltpu.SemaphoreType.DMA,
                pltpu.SemaphoreType.DMA((len(shapes) - n_got,)),
                pltpu.SemaphoreType.DMA((n_dev,)), pltpu.SemaphoreType.DMA((n_dev,))],
            compiler_params=pltpu.CompilerParams(collective_id=0, has_side_effects=True),
            name='exchange',
        )(ao_rows, coeffs)
        got, tiles = outs[:n_got], outs[n_got:]
        moved = {}
        for t in range(len(TILES)):
            for x, k in enumerate(DIAGONAL):
                moved[k, t] = lax.ppermute(
                    tiles[x * len(TILES) + t], 'dev', [(i, i ^ k) for i in range(n_dev)])
        l4 = pl.pallas_call(
            functools.partial(last_kernel, n, rows),
            in_specs=[smem, vmem, hbm],
            out_specs=vmem,
            out_shape=jax.ShapeDtypeStruct(square, BF16),
            name='last',
        )(me_arr, coeffs, got[0])

        out = None
        for t_i, (a0, size, lane, lanes) in enumerate(TILES):
            ins, specs = [], []
            for k in range(n_dev):
                block, at = (moved[k, t_i], (0, 0)) if (k, t_i) in moved else (got[k], (a0, lane))
                ins.append(block)
                specs.append(pl.BlockSpec((pl.Element(rows), pl.Element(8), pl.Element(lanes)), lambda i, at=at: (0, pl.multiple_of(at[0] + 8 * i, 8), at[1])))
            n_in = len(ins)
            ins.append(l4)
            specs.append(const(square))
            if out is not None:
                ins.append(out)
                specs.append(hbm)
            alone = size == 8
            out = pl.pallas_call(
                functools.partial(tail_kernel, n, n_in, a0, lane, lanes, 6) if alone
                else functools.partial(out_kernel, n_in, lanes),
                grid=(size // 8,),
                in_specs=specs,
                out_specs=hbm if alone else pl.BlockSpec(
                    (pl.Element(n), pl.Element(8), pl.Element(lanes)),
                    lambda i, at=(a0, lane): (0, pl.multiple_of(at[0] + 8 * i, 8), at[1])),
                out_shape=jax.ShapeDtypeStruct((n, n, wide), F32),
                input_output_aliases={} if t_i == 0 else {len(ins) - 1: 0},
                scratch_shapes=[pltpu.VMEM((n, 8, lanes), F32), pltpu.SemaphoreType.DMA((6,))] * alone,
                compiler_params=pltpu.CompilerParams(vmem_limit_bytes=67043328),
                name='out',
            )(*ins)
        return out

    return jax.shard_map(transform, mesh=mesh, in_specs=(P(('frag', 'dev')), P('frag')), out_specs=P('frag', None, 'dev'), check_vma=False)
```
